8 devices in a mesh: dp: 2 (over z, y), tp: 4 (over x, core).
Axes of the slice: x: 2, y: 2, z: 1, core: 2. Of those that a mesh axis runs over, the one named last changes fastest.
Arguments:
- x_seq: bfloat16 [3, 256, 5120], P(None, 'dp'), parts along dimension 1
- cache_len: int32 [256], P('dp'), parts along dimension 0
- k_cache: bfloat16 [256, 8, 256, 128], P('dp', 'tp'), parts along dimension 0
- v_cache: bfloat16 [256, 8, 256, 128], P('dp', 'tp'), parts along dimension 0
- w_q: bfloat16 [5120, 5120], P(None, 'tp')
- w_k: bfloat16 [5120, 1024], P(None, 'tp')
- w_v: bfloat16 [5120, 1024], P(None, 'tp')
- w_o: bfloat16 [5120, 5120], P('tp')
- w_gate: bfloat16 [5120, 13824], P(None, 'tp')
- w_up: bfloat16 [5120, 13824], P(None, 'tp')
- w_down: bfloat16 [13824, 5120], P('tp')
- g_q: bfloat16 [5120], P('tp')
- g_k: bfloat16 [1024], P('tp')
- g_attn: bfloat16 [5120], replicated
- g_mlp: bfloat16 [5120], replicated
Outputs:
- output 1: bfloat16 [3, 256, 5120], P(None, 'dp'), parts along dimension 1
- output 2: bfloat16 [256, 8, 256, 128], P('dp', 'tp'), parts along dimension 0
- output 3: bfloat16 [256, 8, 256, 128], P('dp', 'tp'), parts along dimension 0
There are 2 independent parts. The reference program is written for one: setup_inputs(seed, part) draws one part's arguments, and reference() takes and returns one part's arrays. A program takes and returns all parts, laid end to end along the dimension named above; an argument that names none is the same for every part.
All inputs are finite; a program needn't handle non-finite values.
Results may differ from the reference program's by a relative error of at most 0.0196685.
Values are sent between devices in bfloat16 or wider.
A program may use at most 1 GiB of HBM per device.

```python
import math
import jax
import jax.numpy as jnp
from jax import lax

STEPS = 3
MIN_LEN = 128
D_MODEL = 5120
N_HEADS = 40
N_KV_HEADS = 8
HEAD_DIM = 128
FF_DIM = 13824
BATCH_ROWS = 128
MAX_SEQ = 256
ROPE_THETA = 500000.0
NORM_EPS = 1e-6


def draw_lengths(len_key):
    sub_keys = jax.random.split(len_key, 3)
    lengths = jax.random.randint(sub_keys[0], (BATCH_ROWS,), MIN_LEN, MAX_SEQ - STEPS + 1)
    long_row = jax.random.randint(sub_keys[1], (), 0, BATCH_ROWS)
    short_row = (long_row + 1 + jax.random.randint(sub_keys[2], (), 0, BATCH_ROWS - 1)) % BATCH_ROWS
    lengths = lengths.at[long_row].set(MAX_SEQ - STEPS).at[short_row].set(MIN_LEN)
    return lengths.astype(jnp.int32)


def normal_weight(w_key, rows_in, cols_out):
    return jax.random.normal(w_key, (rows_in, cols_out), jnp.float32) * rows_in ** -0.5


def head_scales(scale_key, n_heads):
    log_scale = jax.random.uniform(scale_key, (n_heads,), jnp.float32, math.log(0.3), math.log(3.0))
    return jnp.repeat(jnp.exp(log_scale), HEAD_DIM)


def setup_inputs(seed: int = 0, part: int = 0) -> dict:
    base_key = jax.random.key(seed)
    part_keys = jax.random.split(jax.random.fold_in(base_key, part), 4)
    w_keys = jax.random.split(jax.random.key(seed + 1), 13)
    q_width = N_HEADS * HEAD_DIM
    kv_width = N_KV_HEADS * HEAD_DIM
    cache_shape = (BATCH_ROWS, N_KV_HEADS, MAX_SEQ, HEAD_DIM)
    x_seq = jax.random.normal(part_keys[0], (STEPS, BATCH_ROWS, D_MODEL), jnp.float32)
    k_cache = jax.random.normal(part_keys[2], cache_shape, jnp.float32)
    v_cache = jax.random.normal(part_keys[3], cache_shape, jnp.float32)
    w_q = normal_weight(w_keys[0], D_MODEL, q_width) * head_scales(w_keys[1], N_HEADS)[None, :]
    w_k = normal_weight(w_keys[2], D_MODEL, kv_width) * head_scales(w_keys[3], N_KV_HEADS)[None, :]
    w_v = normal_weight(w_keys[4], D_MODEL, kv_width)
    w_o = normal_weight(w_keys[5], q_width, D_MODEL)
    w_gate = normal_weight(w_keys[6], D_MODEL, FF_DIM)
    w_up = normal_weight(w_keys[7], D_MODEL, FF_DIM)
    w_down = normal_weight(w_keys[8], FF_DIM, D_MODEL)
    g_q = jax.random.uniform(w_keys[9], (q_width,), jnp.float32, 0.5, 1.5)
    g_k = jax.random.uniform(w_keys[10], (kv_width,), jnp.float32, 0.5, 1.5)
    g_attn = jax.random.uniform(w_keys[11], (D_MODEL,), jnp.float32, 0.5, 1.5)
    g_mlp = jax.random.uniform(w_keys[12], (D_MODEL,), jnp.float32, 0.5, 1.5)
    return {'x_seq': x_seq.astype(jnp.bfloat16), 'cache_len': draw_lengths(part_keys[1]), 'k_cache': k_cache.astype(jnp.bfloat16), 'v_cache': v_cache.astype(jnp.bfloat16), 'w_q': w_q.astype(jnp.bfloat16), 'w_k': w_k.astype(jnp.bfloat16), 'w_v': w_v.astype(jnp.bfloat16), 'w_o': w_o.astype(jnp.bfloat16), 'w_gate': w_gate.astype(jnp.bfloat16), 'w_up': w_up.astype(jnp.bfloat16), 'w_down': w_down.astype(jnp.bfloat16), 'g_q': g_q.astype(jnp.bfloat16), 'g_k': g_k.astype(jnp.bfloat16), 'g_attn': g_attn.astype(jnp.bfloat16), 'g_mlp': g_mlp.astype(jnp.bfloat16)}


def rms_factor(sq_sum, full_width):
    return lax.rsqrt(sq_sum / full_width + NORM_EPS)


def rope_tables(positions):
    half_dim = HEAD_DIM // 2
    inv_freq = ROPE_THETA ** (-(jnp.arange(half_dim, dtype=jnp.float32) * (2.0 / HEAD_DIM)))
    angles = positions.astype(jnp.float32)[:, None] * inv_freq[None, :]
    return jnp.cos(angles), jnp.sin(angles)


def apply_rope(head_vals, cos_tab, sin_tab):
    half_dim = HEAD_DIM // 2
    lead_half = head_vals[..., :half_dim]
    tail_half = head_vals[..., half_dim:]
    cos_rows = cos_tab[:, None, :]
    sin_rows = sin_tab[:, None, :]
    return jnp.concatenate([lead_half * cos_rows - tail_half * sin_rows, tail_half * cos_rows + lead_half * sin_rows], axis=-1)


def reference(x_seq, cache_len, k_cache, v_cache, w_q, w_k, w_v, w_o, w_gate, w_up, w_down, g_q, g_k, g_attn, g_mlp):
    q_width = N_HEADS * HEAD_DIM
    kv_width = N_KV_HEADS * HEAD_DIM
    group_size = N_HEADS // N_KV_HEADS
    row_ids = jnp.arange(BATCH_ROWS)
    seq_ids = jnp.arange(MAX_SEQ)
    gain_q = g_q.astype(jnp.float32)
    gain_k = g_k.astype(jnp.float32)
    gain_a = g_attn.astype(jnp.float32)
    gain_m = g_mlp.astype(jnp.float32)

    def attend_row(row_in):
        q_row, k_row, v_row, last_pos = row_in
        q_grp = q_row.reshape(N_KV_HEADS, group_size, HEAD_DIM).astype(jnp.float32)
        scores = jnp.einsum('kgd,ksd->kgs', q_grp, k_row.astype(jnp.float32)) * HEAD_DIM ** -0.5
        scores = jnp.where(seq_ids <= last_pos, scores, -jnp.inf)
        row_max = jnp.max(scores, axis=-1, keepdims=True)
        exp_scores = jnp.exp(scores - row_max)
        row_sum = jnp.sum(exp_scores, axis=-1, keepdims=True)
        mixed_vals = jnp.einsum('kgs,ksd->kgd', exp_scores.astype(jnp.bfloat16).astype(jnp.float32), v_row.astype(jnp.float32))
        return (mixed_vals / row_sum).astype(jnp.bfloat16).reshape(q_width)

    def one_step(cache_pair, step_in):
        k_all, v_all = cache_pair
        x_tok, step_idx = step_in
        positions = cache_len + step_idx
        q_raw = jnp.dot(x_tok, w_q, preferred_element_type=jnp.float32).astype(jnp.bfloat16).astype(jnp.float32)
        k_raw = jnp.dot(x_tok, w_k, preferred_element_type=jnp.float32).astype(jnp.bfloat16).astype(jnp.float32)
        v_new = jnp.dot(x_tok, w_v, preferred_element_type=jnp.float32).astype(jnp.bfloat16).reshape(BATCH_ROWS, N_KV_HEADS, HEAD_DIM)
        q_normed = q_raw * rms_factor(jnp.sum(q_raw * q_raw, axis=-1, keepdims=True), q_width) * gain_q
        k_normed = k_raw * rms_factor(jnp.sum(k_raw * k_raw, axis=-1, keepdims=True), kv_width) * gain_k
        cos_tab, sin_tab = rope_tables(positions)
        q_rot = apply_rope(q_normed.reshape(BATCH_ROWS, N_HEADS, HEAD_DIM), cos_tab, sin_tab).astype(jnp.bfloat16)
        k_rot = apply_rope(k_normed.reshape(BATCH_ROWS, N_KV_HEADS, HEAD_DIM), cos_tab, sin_tab).astype(jnp.bfloat16)
        k_all = k_all.at[row_ids, :, positions, :].set(k_rot)
        v_all = v_all.at[row_ids, :, positions, :].set(v_new)
        attn_vals = lax.map(attend_row, (q_rot, k_all, v_all, positions))
        attn_sum = jnp.dot(attn_vals, w_o, preferred_element_type=jnp.float32).astype(jnp.bfloat16).astype(jnp.float32)
        hidden = (x_tok.astype(jnp.float32) + attn_sum * rms_factor(jnp.sum(attn_sum * attn_sum, axis=-1, keepdims=True), D_MODEL) * gain_a).astype(jnp.bfloat16)
        gate_pre = jnp.dot(hidden, w_gate, preferred_element_type=jnp.float32)
        up_pre = jnp.dot(hidden, w_up, preferred_element_type=jnp.float32)
        act_vals = (jax.nn.silu(gate_pre) * up_pre).astype(jnp.bfloat16)
        mlp_sum = jnp.dot(act_vals, w_down, preferred_element_type=jnp.float32).astype(jnp.bfloat16).astype(jnp.float32)
        y_tok = (hidden.astype(jnp.float32) + mlp_sum * rms_factor(jnp.sum(mlp_sum * mlp_sum, axis=-1, keepdims=True), D_MODEL) * gain_m).astype(jnp.bfloat16)
        return (k_all, v_all), y_tok

    (k_final, v_final), y_seq = lax.scan(one_step, (k_cache, v_cache), (x_seq, jnp.arange(STEPS, dtype=jnp.int32)))
    return (y_seq, k_final, v_final)
```

```python
import functools
import jax
import jax.numpy as jnp
from jax import lax
from jax.experimental import pallas as pl
from jax.experimental.pallas import tpu as pltpu
from jax.sharding import PartitionSpec as P

ROPE_THETA = 500000.0
NORM_EPS = 1e-6
MESH = pl.DeviceIdType.MESH
F32 = jnp.float32
BF16 = jnp.bfloat16

STEPS = 3
BATCH = 128
ROWS = STEPS * BATCH
D_MODEL = 5120
HEAD = 128
KV_LOC = 2
GROUP = 5
Q_LOC = KV_LOC * GROUP
SEQ = 256
FF_LOC = 3456

ANY = pl.BlockSpec(memory_space=pl.ANY)
VM = pl.BlockSpec(memory_space=pltpu.VMEM)
SM = pl.BlockSpec(memory_space=pltpu.SMEM)


N_QKV = 7


def qkv_kernel(x_hbm, wq_hbm, wk_hbm, wv_hbm, gq_ref, gk_ref, cos_ref, sin_ref,
               q_ref, k_ref, v_ref,
               x_v, w_v, raw, q32, sq_own, sq_recv,
               x_sem, w_sem, send_sem, recv_sem):
    me = lax.axis_index('tp')
    barrier = pltpu.get_barrier_semaphore()
    for d in range(1, 4):
        pl.semaphore_signal(barrier, inc=1, device_id={'tp': (me + d) % 4}, device_id_type=MESH)

    x_copy = pltpu.make_async_copy(x_hbm, x_v, x_sem)
    x_copy.start()
    for i in range(5):
        pltpu.make_async_copy(wq_hbm.at[:, pl.ds(i * 256, 256)], w_v.at[i], w_sem.at[i]).start()
    pltpu.make_async_copy(wk_hbm, w_v.at[5], w_sem.at[5]).start()
    pltpu.make_async_copy(wv_hbm, w_v.at[6], w_sem.at[6]).start()
    x_copy.wait()

    def dot_step(i, _):
        pltpu.make_async_copy(wk_hbm, w_v.at[i], w_sem.at[i]).wait()
        res = jnp.dot(x_v[...], w_v[i], preferred_element_type=F32)
        raw[i] = res.astype(BF16).astype(F32)
        return 0

    lax.fori_loop(0, N_QKV, dot_step, 0)

    for t in range(STEPS):
        rows = pl.ds(t * BATCH, BATCH)
        acc = jnp.zeros((BATCH, HEAD), F32)
        for i in range(5):
            for p in range(2):
                piece = raw[i, rows, p * HEAD:(p + 1) * HEAD]
                acc = acc + piece * piece
        q_row = jnp.sum(jnp.transpose(acc), axis=0, keepdims=True)
        acc = jnp.zeros((BATCH, HEAD), F32)
        for p in range(2):
            piece = raw[5, rows, p * HEAD:(p + 1) * HEAD]
            acc = acc + piece * piece
        k_row = jnp.sum(jnp.transpose(acc), axis=0, keepdims=True)
        sq_own[:, t * BATCH:(t + 1) * BATCH] = jnp.concatenate(
            [jnp.broadcast_to(q_row, (8, BATCH)), jnp.broadcast_to(k_row, (8, BATCH))], axis=0)

    pl.semaphore_wait(barrier, 3)
    copies = []
    for d in range(1, 4):
        cp = pltpu.make_async_remote_copy(
            src_ref=sq_own, dst_ref=sq_recv.at[d - 1], send_sem=send_sem.at[d - 1], recv_sem=recv_sem.at[d - 1],
            device_id={'tp': (me + d) % 4}, device_id_type=MESH)
        cp.start()
        copies.append(cp)
    v_ref[...] = raw[6].astype(BF16)
    zero_rows = jnp.zeros((BATCH, HEAD), F32)
    q32[pl.ds(15, BATCH, stride=32), :] = zero_rows
    q32[pl.ds(31, BATCH, stride=32), :] = zero_rows
    for cp in copies:
        cp.wait()

    q_width = float(Q_LOC * HEAD * 4)
    k_width = float(KV_LOC * HEAD * 4)
    for t in range(STEPS):
        cols = slice(t * BATCH, (t + 1) * BATCH)
        rows = pl.ds(t * BATCH, BATCH)
        tot = sq_own[:, cols] + sq_recv[0, :, cols] + sq_recv[1, :, cols] + sq_recv[2, :, cols]
        q_fac = lax.rsqrt(tot[0:1] / q_width + NORM_EPS)
        k_fac = lax.rsqrt(tot[8:9] / k_width + NORM_EPS)
        q_col = jnp.transpose(jnp.broadcast_to(q_fac, (HEAD, BATCH)))
        k_col = jnp.transpose(jnp.broadcast_to(k_fac, (HEAD, BATCH)))
        cos_t = cos_ref[rows, :]
        sin_t = sin_ref[rows, :]
        for hd in range(Q_LOC):
            val = raw[hd // 2, rows, (hd % 2) * HEAD:(hd % 2 + 1) * HEAD]
            val = val * q_col * gq_ref[:, hd * HEAD:(hd + 1) * HEAD]
            rot = val * cos_t + pltpu.roll(val, HEAD // 2, 1) * sin_t
            row = (hd // GROUP) * 16 + t * GROUP + hd % GROUP
            q32[pl.ds(row, BATCH, stride=32), :] = rot
        for kv in range(KV_LOC):
            val = raw[5, rows, kv * HEAD:(kv + 1) * HEAD]
            val = val * k_col * gk_ref[:, kv * HEAD:(kv + 1) * HEAD]
            rot = val * cos_t + pltpu.roll(val, HEAD // 2, 1) * sin_t
            k_ref[rows, kv * HEAD:(kv + 1) * HEAD] = rot.astype(BF16)

    q_ref[...] = q32[...].astype(BF16)


def run_qkv(x2, w_q, w_k, w_v, gq, gk, cos_t, sin_t):
    return pl.pallas_call(
        qkv_kernel,
        out_shape=(jax.ShapeDtypeStruct((BATCH * 32, HEAD), BF16),
                   jax.ShapeDtypeStruct((ROWS, KV_LOC * HEAD), BF16),
                   jax.ShapeDtypeStruct((ROWS, KV_LOC * HEAD), BF16)),
        in_specs=[ANY, ANY, ANY, ANY, VM, VM, VM, VM],
        out_specs=(VM, VM, VM),
        scratch_shapes=[
            pltpu.VMEM((ROWS, D_MODEL), BF16),
            pltpu.VMEM((N_QKV, D_MODEL, 256), BF16),
            pltpu.VMEM((N_QKV, ROWS, 256), F32),
            pltpu.VMEM((BATCH * 32, HEAD), F32),
            pltpu.VMEM((16, ROWS), F32),
            pltpu.VMEM((3, 16, ROWS), F32),
            pltpu.SemaphoreType.DMA,
            pltpu.SemaphoreType.DMA((N_QKV,)),
            pltpu.SemaphoreType.DMA((3,)),
            pltpu.SemaphoreType.DMA((3,)),
        ],
        compiler_params=pltpu.CompilerParams(collective_id=0, has_side_effects=True, vmem_limit_bytes=48 * 1024 * 1024),
        name='qkv_rope',
    )(x2, w_q, w_k, w_v, gq, gk, cos_t, sin_t)


BBLK = 16
N_BLK = BATCH // BBLK
SLOTS = 4


def attn_kernel(len_ref, q_ref, kn_ref, vn_ref, kc_hbm, vc_hbm,
                o_ref, ko_hbm, vo_hbm,
                kbuf, vbuf, o32, in_sem, out_sem):
    def in_copy(i, s, which):
        src = (kc_hbm, vc_hbm)[which]
        dst = (kbuf, vbuf)[which]
        return pltpu.make_async_copy(src.at[pl.ds(i * BBLK, BBLK)], dst.at[s], in_sem.at[which, s])

    def out_copy(i, s, which):
        dst = (ko_hbm, vo_hbm)[which]
        src = (kbuf, vbuf)[which]
        return pltpu.make_async_copy(src.at[s], dst.at[pl.ds(i * BBLK, BBLK)], out_sem.at[which, s])

    for i in range(2):
        in_copy(i, i, 0).start()
        in_copy(i, i, 1).start()

    scale = HEAD ** -0.5
    row_id = lax.broadcasted_iota(jnp.int32, (32, SEQ), 0)
    col_id = lax.broadcasted_iota(jnp.int32, (32, SEQ), 1)
    sub = row_id - jnp.where(row_id >= 16, 16, 0)
    step_of = jnp.where(sub >= 5, 1, 0) + jnp.where(sub >= 10, 1, 0)
    gap = col_id - step_of
    win_id = lax.broadcasted_iota(jnp.int32, (32, HEAD), 0)

    def block(i, _):
        s = i % SLOTS

        @pl.when(i >= 2)
        def _():
            out_copy(i - 2, (i + 2) % SLOTS, 0).wait()
            out_copy(i - 2, (i + 2) % SLOTS, 1).wait()

        @pl.when(i + 2 < N_BLK)
        def _():
            in_copy(i + 2, (i + 2) % SLOTS, 0).start()
            in_copy(i + 2, (i + 2) % SLOTS, 1).start()

        in_copy(i, s, 0).wait()
        in_copy(i, s, 1).wait()

        news = []
        for src in (kn_ref, vn_ref):
            news.append([src[pl.ds(pl.multiple_of(t * BATCH + i * BBLK, BBLK), BBLK), :].astype(F32) for t in range(STEPS)])
        for bl in range(BBLK):
            ln = len_ref[i * BBLK + bl]
            w0 = jnp.minimum((ln // 16) * 16, SEQ - 32)
            win = pl.ds(pl.multiple_of(w0, 16), 32)
            rel = win_id - (ln - w0)
            for buf, new in ((kbuf, news[0]), (vbuf, news[1])):
                for kv in range(KV_LOC):
                    val = buf[s, bl, kv, win, :].astype(F32)
                    for t in range(STEPS):
                        row = new[t][bl:bl + 1, kv * HEAD:(kv + 1) * HEAD]
                        val = jnp.where(rel == t, jnp.broadcast_to(row, (32, HEAD)), val)
                    buf[s, bl, kv, win, :] = val.astype(BF16)
        out_copy(i, s, 0).start()
        out_copy(i, s, 1).start()

        zero_q = jnp.zeros((16, HEAD), BF16)
        for bl in range(BBLK):
            ln = len_ref[i * BBLK + bl]
            q_b = q_ref[pl.ds(pl.multiple_of((i * BBLK + bl) * 32, 32), 32), :]
            lhs = jnp.concatenate([jnp.concatenate([q_b[:16], zero_q], axis=1),
                                   jnp.concatenate([zero_q, q_b[16:]], axis=1)], axis=0)
            k_cat = jnp.concatenate([kbuf[s, bl, 0], kbuf[s, bl, 1]], axis=1)
            v_cat = jnp.concatenate([vbuf[s, bl, 0], vbuf[s, bl, 1]], axis=1)
            sc = lax.dot_general(lhs, k_cat, (((1,), (1,)), ((), ())), preferred_element_type=F32) * scale
            sc = jnp.where(gap <= ln, sc, -jnp.inf)
            top = jnp.max(sc, axis=1, keepdims=True)
            ex = jnp.exp(sc - top)
            den = jnp.sum(ex, axis=1, keepdims=True)
            mix = jnp.dot(ex.astype(BF16), v_cat, preferred_element_type=F32)
            o32[bl * 32:bl * 32 + 16, :] = mix[:16, :HEAD] / den[:16]
            o32[bl * 32 + 16:bl * 32 + 32, :] = mix[16:, HEAD:] / den[16:]
        for t in range(STEPS):
            for hd in range(Q_LOC):
                row = (hd // GROUP) * 16 + t * GROUP + hd % GROUP
                slab = o32[pl.ds(row, BBLK, stride=32), :]
                o_ref[t, pl.ds(pl.multiple_of(i * BBLK, BBLK), BBLK), hd * HEAD:(hd + 1) * HEAD] = slab.astype(BF16)
        return 0

    lax.fori_loop(0, N_BLK, block, 0)
    for i in range(N_BLK - 2, N_BLK):
        out_copy(i, i % SLOTS, 0).wait()
        out_copy(i, i % SLOTS, 1).wait()


def run_attn(lengths, q32, k_new, v_new, k_cache, v_cache):
    return pl.pallas_call(
        attn_kernel,
        out_shape=(jax.ShapeDtypeStruct((STEPS, BATCH, Q_LOC * HEAD), BF16),
                   jax.ShapeDtypeStruct(k_cache.shape, BF16),
                   jax.ShapeDtypeStruct(v_cache.shape, BF16)),
        in_specs=[SM, VM, VM, VM, ANY, ANY],
        out_specs=(VM, ANY, ANY),
        scratch_shapes=[
            pltpu.VMEM((SLOTS, BBLK, KV_LOC, SEQ, HEAD), BF16),
            pltpu.VMEM((SLOTS, BBLK, KV_LOC, SEQ, HEAD), BF16),
            pltpu.VMEM((BBLK * 32, HEAD), F32),
            pltpu.SemaphoreType.DMA((2, SLOTS)),
            pltpu.SemaphoreType.DMA((2, SLOTS)),
        ],
        compiler_params=pltpu.CompilerParams(vmem_limit_bytes=48 * 1024 * 1024),
        name='attend',
    )(lengths, q32, k_new, v_new, k_cache, v_cache)


CHUNKS = (64, 64)
CROWS = tuple(STEPS * n for n in CHUNKS)
PIECES = 10
PW = 256
HALF_T = PIECES
RING = 5
RESID = 9
G_TILES = FF_LOC // 128
G_STREAM = G_TILES - RESID
PHASES = (('w', 2 * PIECES), ('g', G_STREAM), ('d', 2 * PIECES), ('g', G_STREAM), ('d', 2 * PIECES))


def mlp_kernel(o_hbm, x_hbm, wo_hbm, w1_hbm, w3_hbm, w2_hbm, ga_ref, gm_ref,
               y_hbm,
               o_v, xh0, xh1, u0, u1, ps0, ps1, pr0, pr1, s0, s1, r10, r11, r20, r21, a0, a1, ring,
               in_sem, ring_sem, res_sem, out_sem,
               p_send, p_recv, c_send, c_recv, a_send, a_recv):
    me = lax.axis_index('tp')
    core = me % 2
    chip = me // 2
    mate = chip * 2 + (1 - core)
    peer = (1 - chip) * 2 + core
    xh, u_v = (xh0, xh1), (u0, u1)
    p_out, p_in, s_v = (ps0, ps1), (pr0, pr1), (s0, s1)
    r_v = ((r10, r11), (r20, r21))
    a_v = (a0, a1)
    firsts = (0, CHUNKS[0])
    row0 = (0, CROWS[0])

    barrier = pltpu.get_barrier_semaphore()
    for dev in (mate, peer):
        pl.semaphore_signal(barrier, inc=1, device_id={'tp': dev}, device_id_type=MESH)

    bases = []
    total = 0
    for _, n in PHASES:
        bases.append(total)
        total += n

    def out_col(i):
        k = i // 2
        own = i % 2
        half = own * core + (1 - own) * (1 - core)
        return half * HALF_T + k

    def g_tile(s):
        return (s // 2) * 3 + s % 2

    def tile_copies(kind, idx, slot, sem):
        if kind == 'w':
            col = pl.multiple_of(out_col(idx) * PW, PW)
            return [pltpu.make_async_copy(wo_hbm.at[:, pl.ds(col, PW)], ring.at[slot, pl.ds(0, Q_LOC * HEAD), :], sem.at[0])]
        if kind == 'd':
            col = pl.multiple_of(out_col(idx) * PW, PW)
            return [pltpu.make_async_copy(w2_hbm.at[:, pl.ds(col, PW)], ring.at[slot, pl.ds(0, FF_LOC), :], sem.at[0])]
        col = pl.multiple_of(idx * 128, 128)
        return [pltpu.make_async_copy(w1_hbm.at[:, pl.ds(col, 128)], ring.at[slot, :, pl.ds(0, 128)], sem.at[0]),
                pltpu.make_async_copy(w3_hbm.at[:, pl.ds(col, 128)], ring.at[slot, :, pl.ds(128, 128)], sem.at[1])]

    def stream(ph, s, start):
        kind = PHASES[ph][0]
        slot = (bases[ph] + s) % RING
        idx = g_tile(s) if kind == 'g' else s
        for cp in tile_copies(kind, idx, slot, ring_sem.at[slot]):
            if start:
                cp.start()
            else:
                cp.wait()
        return slot

    def refill(ph, s):
        n = PHASES[ph][1]

        @pl.when(s + RING < n)
        def _():
            stream(ph, s + RING, True)

        if ph + 1 < len(PHASES):
            @pl.when(s + RING >= n)
            def _():
                stream(ph + 1, s + RING - n, True)

    o_copies, x_copies = [], []
    for ch in range(2):
        for t in range(STEPS):
            o_copies.append(pltpu.make_async_copy(
                o_hbm.at[t, pl.ds(firsts[ch], CHUNKS[ch]), :],
                o_v.at[pl.ds(row0[ch] + t * CHUNKS[ch], CHUNKS[ch]), :], in_sem.at[0, ch, t]))
            x_copies.append(pltpu.make_async_copy(
                x_hbm.at[t, pl.ds(firsts[ch], CHUNKS[ch]), :],
                xh[ch].at[pl.ds(t * CHUNKS[ch], CHUNKS[ch]), :], in_sem.at[1, ch, t]))
    for cp in o_copies:
        cp.start()
    for n in range(RING):
        stream(0, n, True)
    for cp in x_copies:
        cp.start()

    def mate_copy(ex, ch, k):
        return pltpu.make_async_remote_copy(
            src_ref=p_out[ch].at[k], dst_ref=p_in[ch].at[k], send_sem=p_send.at[ex, ch, k], recv_sem=p_recv.at[ex, ch, k],
            device_id={'tp': mate}, device_id_type=MESH)

    def peer_copy(ex, ch, k):
        return pltpu.make_async_remote_copy(
            src_ref=s_v[ch].at[k], dst_ref=r_v[ex][ch].at[k], send_sem=c_send.at[ex, ch, k], recv_sem=c_recv.at[ex, ch, k],
            device_id={'tp': peer}, device_id_type=MESH)

    def gather_copy(ex, ch, k, half):
        j = half * HALF_T + k
        return pltpu.make_async_remote_copy(
            src_ref=a_v[ch].at[j], dst_ref=a_v[ch].at[j], send_sem=a_send.at[ex, ch, k], recv_sem=a_recv.at[ex, ch, k],
            device_id={'tp': mate}, device_id_type=MESH)

    def pair_sum(ex, ch, k):
        mate_copy(ex, ch, k).wait_recv()
        s_v[ch][k] = (s_v[ch][k].astype(F32) + p_in[ch][k].astype(F32)).astype(BF16)

    def full_sum(ex, ch, k):
        peer_copy(ex, ch, k).wait()
        a_v[ch][core * HALF_T + k] = (s_v[ch][k].astype(F32) + r_v[ex][ch][k].astype(F32)).astype(BF16)
        gather_copy(ex, ch, k, core).start()

    def gather_done(ex, ch):
        def step(k, _):
            gather_copy(ex, ch, k, core).wait_send()
            gather_copy(ex, ch, k, 1 - core).wait_recv()
            mate_copy(ex, ch, k).wait_send()
            return 0
        lax.fori_loop(0, PIECES, step, 0)

    def full_sums(ex, ch):
        def step(k, _):
            full_sum(ex, ch, k)
            return 0
        lax.fori_loop(0, PIECES, step, 0)

    def norm_add(ch, gain_ref):
        def step(b, _):
            rows = pl.ds(pl.multiple_of(b * 16, 16), 16)
            acc = jnp.zeros((16, PW), F32)
            for j in range(2 * PIECES):
                val = a_v[ch][j, rows, :].astype(F32)
                acc = acc + val * val
            fac = lax.rsqrt(jnp.sum(acc, axis=1, keepdims=True) / float(D_MODEL) + NORM_EPS)
            for j in range(2 * PIECES):
                cols = slice(j * PW, (j + 1) * PW)
                val = a_v[ch][j, rows, :].astype(F32)
                base = xh[ch][rows, cols].astype(F32)
                xh[ch][rows, cols] = (base + val * fac * gain_ref[:, cols]).astype(BF16)
            return 0
        lax.fori_loop(0, CROWS[ch] // 16, step, 0)

    for cp in o_copies:
        cp.wait()

    def wo_tile(i):
        slot = stream(0, i, False)
        res = jnp.dot(o_v[...], ring[slot, pl.ds(0, Q_LOC * HEAD), :], preferred_element_type=F32).astype(BF16)
        refill(0, i)
        return res

    def wo_step(k, _):
        res = wo_tile(2 * k)
        for ch in range(2):
            p_out[ch][k] = res[row0[ch]:row0[ch] + CROWS[ch]]
            mate_copy(0, ch, k).start()
        res = wo_tile(2 * k + 1)
        for ch in range(2):
            s_v[ch][k] = res[row0[ch]:row0[ch] + CROWS[ch]]

        @pl.when(k >= 1)
        def _():
            pair_sum(0, 0, k - 1)
            peer_copy(0, 0, k - 1).start()
            pair_sum(0, 1, k - 1)
        return 0

    pl.semaphore_wait(barrier, 2)
    lax.fori_loop(0, PIECES, wo_step, 0)
    pair_sum(0, 0, PIECES - 1)
    peer_copy(0, 0, PIECES - 1).start()
    pair_sum(0, 1, PIECES - 1)

    def send_b(k, _):
        peer_copy(0, 1, k).start()
        return 0
    lax.fori_loop(0, PIECES, send_b, 0)

    def res_load(r, _):
        for cp in tile_copies('g', r * 3 + 2, RING + r, res_sem.at[r]):
            cp.start()
        return 0
    lax.fori_loop(0, RESID, res_load, 0)
    for cp in x_copies:
        cp.wait()

    full_sums(0, 0)
    gather_done(0, 0)
    norm_add(0, ga_ref)

    def res_wait(r, _):
        for cp in tile_copies('g', r * 3 + 2, RING + r, res_sem.at[r]):
            cp.wait()
        return 0
    lax.fori_loop(0, RESID, res_wait, 0)

    def gate_up(ph, ch):
        def tile(i, slot):
            acc = jnp.dot(xh[ch][...], ring[slot], preferred_element_type=F32)
            gate = acc[:, :128]
            act = (gate * jax.nn.sigmoid(gate)) * acc[:, 128:]
            u_v[ch][:, pl.ds(pl.multiple_of(i * 128, 128), 128)] = act.astype(BF16)

        def step(i, _):
            q = i // 3
            m = i % 3
            s = 2 * q + m

            @pl.when(m < 2)
            def _():
                stream(ph, s, False)
            slot = jnp.where(m == 2, RING + q, (bases[ph] + s) % RING)
            tile(i, slot)

            @pl.when(m < 2)
            def _():
                refill(ph, s)
            return 0
        lax.fori_loop(0, G_TILES, step, 0)

    def down(ph, ch, also):
        def d_tile(i):
            slot = stream(ph, i, False)
            res = jnp.dot(u_v[ch][...], ring[slot, pl.ds(0, FF_LOC), :], preferred_element_type=F32).astype(BF16)
            refill(ph, i)
            return res

        def step(k, _):
            p_out[ch][k] = d_tile(2 * k)
            mate_copy(1, ch, k).start()
            s_v[ch][k] = d_tile(2 * k + 1)

            @pl.when(k >= 1)
            def _():
                pair_sum(1, ch, k - 1)
                peer_copy(1, ch, k - 1).start()
            if also is not None:
                also(k)
            return 0
        lax.fori_loop(0, PIECES, step, 0)
        pair_sum(1, ch, PIECES - 1)
        peer_copy(1, ch, PIECES - 1).start()

    gate_up(1, 0)
    down(2, 0, lambda k: full_sum(0, 1, k))
    gather_done(0, 1)
    norm_add(1, ga_ref)
    gate_up(3, 1)
    down(4, 1, lambda k: full_sum(1, 0, k))

    def y_copies(ch):
        return [pltpu.make_async_copy(xh[ch].at[pl.ds(t * CHUNKS[ch], CHUNKS[ch]), :],
                                      y_hbm.at[t, pl.ds(firsts[ch], CHUNKS[ch]), :], out_sem.at[ch, t]) for t in range(STEPS)]

    gather_done(1, 0)
    norm_add(0, gm_ref)
    for cp in y_copies(0):
        cp.start()
    full_sums(1, 1)
    gather_done(1, 1)
    norm_add(1, gm_ref)
    for cp in y_copies(1):
        cp.start()
    for ch in range(2):
        for cp in y_copies(ch):
            cp.wait()


def run_mlp(o, x_seq, w_o, w_gate, w_up, w_down, ga, gm):
    piece = lambda ch: pltpu.VMEM((PIECES, CROWS[ch], PW), BF16)
    sem = pltpu.SemaphoreType.DMA
    return pl.pallas_call(
        mlp_kernel,
        out_shape=jax.ShapeDtypeStruct((STEPS, BATCH, D_MODEL), BF16),
        in_specs=[ANY, ANY, ANY, ANY, ANY, ANY, VM, VM],
        out_specs=ANY,
        scratch_shapes=[
            pltpu.VMEM((ROWS, Q_LOC * HEAD), BF16),
            pltpu.VMEM((CROWS[0], D_MODEL), BF16), pltpu.VMEM((CROWS[1], D_MODEL), BF16),
            pltpu.VMEM((CROWS[0], FF_LOC), BF16), pltpu.VMEM((CROWS[1], FF_LOC), BF16),
            piece(0), piece(1), piece(0), piece(1), piece(0), piece(1),
            piece(0), piece(1), piece(0), piece(1),
            pltpu.VMEM((2 * PIECES, CROWS[0], PW), BF16), pltpu.VMEM((2 * PIECES, CROWS[1], PW), BF16),
            pltpu.VMEM((RING + RESID, D_MODEL, PW), BF16),
            sem((2, 2, STEPS)), sem((RING, 2)), sem((RESID, 2)), sem((2, STEPS)),
            sem((2, 2, PIECES)), sem((2, 2, PIECES)), sem((2, 2, PIECES)),
            sem((2, 2, PIECES)), sem((2, 2, PIECES)), sem((2, 2, PIECES)),
        ],
        compiler_params=pltpu.CompilerParams(collective_id=1, has_side_effects=True, vmem_limit_bytes=67043328),
        name='wo_mlp',
    )(o, x_seq, w_o, w_gate, w_up, w_down, ga, gm)


def solution(mesh):
    def local_run(x_seq, cache_len, k_cache, v_cache, w_q, w_k, w_v, w_o, w_gate, w_up, w_down, g_q, g_k, g_attn, g_mlp):
        inv_freq = ROPE_THETA ** (-(jnp.arange(HEAD // 2, dtype=F32) * (2.0 / HEAD)))
        pos = (cache_len[None, :] + jnp.arange(STEPS, dtype=jnp.int32)[:, None]).reshape(ROWS)
        ang = pos.astype(F32)[:, None] * jnp.concatenate([inv_freq, inv_freq])[None, :]
        cos_t = jnp.cos(ang)
        sin_t = jnp.sin(ang) * jnp.where(jnp.arange(HEAD) < HEAD // 2, -1.0, 1.0).astype(F32)[None, :]
        row = lambda g: g.astype(F32)[None, :]
        q32, k_new, v_new = run_qkv(x_seq.reshape(ROWS, D_MODEL), w_q, w_k, w_v, row(g_q), row(g_k), cos_t, sin_t)
        o, k_out, v_out = run_attn(cache_len, q32, k_new, v_new, k_cache, v_cache)
        y = run_mlp(o, x_seq, w_o, w_gate, w_up, w_down, row(g_attn), row(g_mlp))
        return y, k_out, v_out

    data_spec = P(None, 'dp', None)
    cache_spec = P('dp', 'tp', None, None)
    col_spec = P(None, 'tp')
    row_spec = P('tp', None)
    arg_specs = (data_spec, P('dp'), cache_spec, cache_spec, col_spec, col_spec, col_spec, row_spec, col_spec, col_spec, row_spec, P('tp'), P('tp'), P(None), P(None))
    out_specs = (data_spec, cache_spec, cache_spec)
    return jax.shard_map(local_run, mesh=mesh, in_specs=arg_specs, out_specs=out_specs, check_vma=False)
```

```python
import jax
import jax.numpy as jnp
import numpy as np
from jax import lax
from jax.experimental import pallas as pl
from jax.experimental.pallas import tpu as pltpu
from jax.sharding import PartitionSpec as P

ROPE_THETA = 500000.0
NORM_EPS = 1e-6
MESH = pl.DeviceIdType.MESH
F32 = jnp.float32
BF16 = jnp.bfloat16

STEPS = 3
BATCH = 128
ROWS = STEPS * BATCH
D_MODEL = 5120
HEAD = 128
KV_LOC = 2
GROUP = 5
Q_LOC = KV_LOC * GROUP
SEQ = 256
FF_LOC = 3456

ANY = pl.BlockSpec(memory_space=pl.ANY)
VM = pl.BlockSpec(memory_space=pltpu.VMEM)
SM = pl.BlockSpec(memory_space=pltpu.SMEM)
HB = pl.BlockSpec(memory_space=pltpu.HBM)


N_TILE = 512


def qkv_kernel(x_hbm, wq_hbm, wk_hbm, wv_hbm, gq_hbm, gk_hbm, len_hbm, freq_hbm,
               q_hbm, k_hbm, v_hbm,
               x_v, w_v, raw, cos_v, sin_v, sq_acc, sq_own, sq_recv, q_v, k_v, v_v, gq_v, gk_v, len_v, freq_v,
               x_sem, w_sem, send_sem, recv_sem, t_sem, o_sem):
    me = lax.axis_index('tp')
    barrier = pltpu.get_barrier_semaphore()
    for d in range(1, 4):
        pl.semaphore_signal(barrier, inc=1, device_id={'tp': (me + d) % 4}, device_id_type=MESH)

    half_k = D_MODEL // 2
    halves = [pl.ds(n * half_k, half_k) for n in range(2)]
    x_copies = [pltpu.make_async_copy(x_hbm.at[:, h], x_v.at[:, h], x_sem.at[n]) for n, h in enumerate(halves)]
    w_copies = [
        [pltpu.make_async_copy(wq_hbm.at[h, pl.ds(0, 512)], w_v.at[0, h], w_sem.at[n]) for n, h in enumerate(halves)],
        [pltpu.make_async_copy(wq_hbm.at[:, pl.ds(512, 512)], w_v.at[1], w_sem.at[2])],
        [pltpu.make_async_copy(wq_hbm.at[:, pl.ds(1024, 256)], w_v.at[2, :, pl.ds(0, 256)], w_sem.at[3]),
         pltpu.make_async_copy(wk_hbm, w_v.at[2, :, pl.ds(256, 256)], w_sem.at[4])],
        [pltpu.make_async_copy(wv_hbm, w_v.at[3, :, pl.ds(0, 256)], w_sem.at[5])],
    ]
    t_copies = [pltpu.make_async_copy(src, dst, t_sem.at[n])
                for n, (src, dst) in enumerate(((len_hbm, len_v), (freq_hbm, freq_v), (gq_hbm, gq_v), (gk_hbm, gk_v)))]
    for cp in t_copies:
        cp.start()
    for n in range(2):
        x_copies[n].start()
        w_copies[0][n].start()

    for cp in t_copies:
        cp.wait()
    len_col = jnp.transpose(jnp.broadcast_to(len_v[...].astype(F32), (HEAD, BATCH)))
    sign = jnp.where(lax.broadcasted_iota(jnp.int32, (BATCH, HEAD), 1) < HEAD // 2, -1.0, 1.0)
    for t in range(STEPS):
        rows = pl.ds(t * BATCH, BATCH)
        ang = (len_col + float(t)) * freq_v[...]
        cos_v[rows, :] = jnp.cos(ang)
        sin_v[rows, :] = jnp.sin(ang) * sign

    def piece(col, rows):
        return raw[col // N_TILE, rows, col % N_TILE:col % N_TILE + HEAD]

    def square(cols, rows, acc):
        for col in cols:
            val = piece(col, rows)
            acc = acc + val * val
        return acc

    all_rows = [pl.ds(t * BATCH, BATCH) for t in range(STEPS)]
    zero = jnp.zeros((BATCH, HEAD), F32)

    with jax.named_scope('k1_w0'):
        x_copies[0].wait()
        w_copies[0][0].wait()
    w_copies[1][0].start()
    part = jnp.dot(x_v[:, halves[0]], w_v[0, halves[0], :], preferred_element_type=F32)
    raw[0] = part
    x_copies[1].wait()
    w_copies[0][1].wait()
    for cp in w_copies[2]:
        cp.start()
    part = jnp.dot(x_v[:, halves[1]], w_v[0, halves[1], :], preferred_element_type=F32)
    raw[0] = (raw[0] + part).astype(BF16).astype(F32)
    w_copies[1][0].wait()
    w_copies[3][0].start()
    raw[1] = jnp.dot(x_v[...], w_v[1], preferred_element_type=F32).astype(BF16).astype(F32)
    w_copies[2][0].wait()
    w_copies[2][1].wait()
    for t in range(STEPS):
        sq_acc[all_rows[t], :] = square(range(0, 1024, HEAD), all_rows[t], zero)
    raw[2] = jnp.dot(x_v[...], w_v[2], preferred_element_type=F32).astype(BF16).astype(F32)
    w_copies[3][0].wait()

    first_row = lax.broadcasted_iota(jnp.int32, (8, BATCH), 0) == 0
    for t in range(STEPS):
        rows = all_rows[t]
        sums = [jnp.sum(jnp.transpose(acc), axis=0, keepdims=True)
                for acc in (square(range(1024, 1280, HEAD), rows, sq_acc[rows, :]), square(range(1280, 1536, HEAD), rows, zero))]
        sq_own[:, t * BATCH:(t + 1) * BATCH] = jnp.where(first_row, sums[0], sums[1])

    with jax.named_scope('k1_barrier'):
        pl.semaphore_wait(barrier, 3)
    copies = []
    for d in range(1, 4):
        cp = pltpu.make_async_remote_copy(
            src_ref=sq_own, dst_ref=sq_recv.at[d - 1], send_sem=send_sem.at[d - 1], recv_sem=recv_sem.at[d - 1],
            device_id={'tp': (me + d) % 4}, device_id_type=MESH)
        cp.start()
        copies.append(cp)
    v_v[...] = jnp.dot(x_v[...], w_v[3, :, pl.ds(0, 256)], preferred_element_type=F32).astype(BF16)
    outs = [pltpu.make_async_copy(v_v, v_hbm, o_sem.at[0])]
    outs[0].start()
    with jax.named_scope('k1_recv'):
        for cp in copies:
            cp.wait()

    q_width = float(Q_LOC * HEAD * 4)
    k_width = float(KV_LOC * HEAD * 4)
    for t in range(STEPS):
        cols = slice(t * BATCH, (t + 1) * BATCH)
        rows = all_rows[t]
        tot = sq_own[:, cols] + sq_recv[0, :, cols] + sq_recv[1, :, cols] + sq_recv[2, :, cols]
        q_fac = lax.rsqrt(tot[0:1] / q_width + NORM_EPS)
        k_fac = lax.rsqrt(tot[1:2] / k_width + NORM_EPS)
        q_col = jnp.transpose(jnp.broadcast_to(q_fac, (HEAD, BATCH)))
        k_col = jnp.transpose(jnp.broadcast_to(k_fac, (HEAD, BATCH)))
        cos_t = cos_v[rows, :]
        sin_t = sin_v[rows, :]
        for hd in range(Q_LOC):
            val = piece(hd * HEAD, rows) * q_col * gq_v[hd:hd + 1, :].astype(F32)
            rot = val * cos_t + pltpu.roll(val, HEAD // 2, 1) * sin_t
            q_v[(hd // GROUP) * 15 + t * GROUP + hd % GROUP] = rot.astype(BF16)
        for kv in range(KV_LOC):
            val = piece((Q_LOC + kv) * HEAD, rows) * k_col * gk_v[kv:kv + 1, :].astype(F32)
            rot = val * cos_t + pltpu.roll(val, HEAD // 2, 1) * sin_t
            k_v[rows, kv * HEAD:(kv + 1) * HEAD] = rot.astype(BF16)
        for kv in range(KV_LOC):
            slabs = pl.ds(kv * 15 + t * GROUP, GROUP)
            outs.append(pltpu.make_async_copy(q_v.at[slabs], q_hbm.at[slabs], o_sem.at[len(outs)]))
        outs.append(pltpu.make_async_copy(k_v.at[rows], k_hbm.at[rows], o_sem.at[len(outs)]))
        for cp in outs[-3:]:
            cp.start()
    with jax.named_scope('k1_out'):
        for cp in outs:
            cp.wait()


def run_qkv(x2, w_q, w_k, w_v, g_q, g_k, len_row, freq_row):
    return pl.pallas_call(
        qkv_kernel,
        out_shape=(jax.ShapeDtypeStruct((30, BATCH, HEAD), BF16),
                   jax.ShapeDtypeStruct((ROWS, KV_LOC * HEAD), BF16),
                   jax.ShapeDtypeStruct((ROWS, KV_LOC * HEAD), BF16)),
        in_specs=[HB] * 8,
        out_specs=(HB, HB, HB),
        scratch_shapes=[
            pltpu.VMEM((ROWS, D_MODEL), BF16),
            pltpu.VMEM((4, D_MODEL, N_TILE), BF16),
            pltpu.VMEM((3, ROWS, N_TILE), F32),
            pltpu.VMEM((ROWS, HEAD), F32),
            pltpu.VMEM((ROWS, HEAD), F32),
            pltpu.VMEM((ROWS, HEAD), F32),
            pltpu.VMEM((8, ROWS), F32),
            pltpu.VMEM((3, 8, ROWS), F32),
            pltpu.VMEM((30, BATCH, HEAD), BF16),
            pltpu.VMEM((ROWS, KV_LOC * HEAD), BF16),
            pltpu.VMEM((ROWS, KV_LOC * HEAD), BF16),
            pltpu.VMEM((Q_LOC, HEAD), BF16),
            pltpu.VMEM((KV_LOC, HEAD), BF16),
            pltpu.VMEM((1, BATCH), jnp.int32),
            pltpu.VMEM((1, HEAD), F32),
            pltpu.SemaphoreType.DMA((2,)),
            pltpu.SemaphoreType.DMA((6,)),
            pltpu.SemaphoreType.DMA((3,)),
            pltpu.SemaphoreType.DMA((3,)),
            pltpu.SemaphoreType.DMA((4,)),
            pltpu.SemaphoreType.DMA((10,)),
        ],
        compiler_params=pltpu.CompilerParams(collective_id=0, has_side_effects=True, vmem_limit_bytes=67043328),
        name='qkv_rope',
    )(x2, w_q, w_k, w_v, g_q, g_k, len_row, freq_row)


BBLK = 16
N_BLK = BATCH // BBLK
SLOTS = 4


def attn_kernel(len_ref, q_hbm, kn_hbm, vn_hbm, kc_hbm, vc_hbm,
                o_hbm, ko_hbm, vo_hbm,
                kbuf, vbuf, q32, o32, sc_v, ex_v, den_v, o_buf, q_ref, kn_ref, vn_ref, in_sem, out_sem, o_sem, t_sem):
    def in_copy(i, s, which):
        src = (kc_hbm, vc_hbm)[which]
        dst = (kbuf, vbuf)[which]
        return pltpu.make_async_copy(src.at[pl.ds(i * BBLK, BBLK)], dst.at[s], in_sem.at[which, s])

    def out_copy(i, s, which):
        dst = (ko_hbm, vo_hbm)[which]
        src = (kbuf, vbuf)[which]
        return pltpu.make_async_copy(src.at[s], dst.at[pl.ds(i * BBLK, BBLK)], out_sem.at[which, s])

    def o_copy(i, t):
        return pltpu.make_async_copy(o_buf.at[i % 2, t], o_hbm.at[t, pl.ds(pl.multiple_of(i * BBLK, BBLK), BBLK), :], o_sem.at[i % 2, t])

    t_copies = [pltpu.make_async_copy(src, dst, t_sem.at[n])
                for n, (src, dst) in enumerate(((kn_hbm, kn_ref), (vn_hbm, vn_ref), (q_hbm, q_ref)))]
    for cp in t_copies:
        cp.start()
    for i in range(2):
        in_copy(i, i, 0).start()
        in_copy(i, i, 1).start()
    for pad in (15, 31):
        q32[pl.ds(pad, BBLK, stride=32), :] = jnp.zeros((BBLK, HEAD), F32)

    scale = HEAD ** -0.5
    row_id = lax.broadcasted_iota(jnp.int32, (32, SEQ), 0)
    col_id = lax.broadcasted_iota(jnp.int32, (32, SEQ), 1)
    sub = row_id - jnp.where(row_id >= 16, 16, 0)
    step_of = jnp.where(sub >= 5, 1, 0) + jnp.where(sub >= 10, 1, 0)
    gap = col_id - step_of
    win_id = lax.broadcasted_iota(jnp.int32, (32, HEAD), 0)

    for cp in t_copies:
        cp.wait()

    def block(i, _):
        s = i % SLOTS

        @pl.when(i >= 2)
        def _():
            out_copy(i - 2, (i + 2) % SLOTS, 0).wait()
            out_copy(i - 2, (i + 2) % SLOTS, 1).wait()
            for t in range(STEPS):
                o_copy(i - 2, t).wait()

        @pl.when(i + 2 < N_BLK)
        def _():
            in_copy(i + 2, (i + 2) % SLOTS, 0).start()
            in_copy(i + 2, (i + 2) % SLOTS, 1).start()

        in_copy(i, s, 0).wait()
        in_copy(i, s, 1).wait()

        news = []
        for src in (kn_ref, vn_ref):
            news.append([src[pl.ds(pl.multiple_of(t * BATCH + i * BBLK, BBLK), BBLK), :].astype(F32) for t in range(STEPS)])
        for bl in range(BBLK):
            ln = len_ref[i * BBLK + bl]
            w0 = jnp.minimum((ln // 16) * 16, SEQ - 32)
            win = pl.ds(pl.multiple_of(w0, 16), 32)
            rel = win_id - (ln - w0)
            for buf, new in ((kbuf, news[0]), (vbuf, news[1])):
                for kv in range(KV_LOC):
                    val = buf[s, bl, kv, win, :].astype(F32)
                    for t in range(STEPS):
                        row = new[t][bl:bl + 1, kv * HEAD:(kv + 1) * HEAD]
                        val = jnp.where(rel == t, jnp.broadcast_to(row, (32, HEAD)), val)
                    buf[s, bl, kv, win, :] = val.astype(BF16)
        out_copy(i, s, 0).start()
        out_copy(i, s, 1).start()

        zero_q = jnp.zeros((16, HEAD), BF16)
        for row in range(30):
            q32[pl.ds(row + row // 15, BBLK, stride=32), :] = q_ref[row, pl.ds(pl.multiple_of(i * BBLK, BBLK), BBLK), :].astype(F32)
        for bl in range(BBLK):
            ln = len_ref[i * BBLK + bl]
            q_b = q32[bl * 32:(bl + 1) * 32, :].astype(BF16)
            lhs = jnp.concatenate([jnp.concatenate([q_b[:16], zero_q], axis=1),
                                   jnp.concatenate([zero_q, q_b[16:]], axis=1)], axis=0)
            k_cat = jnp.concatenate([kbuf[s, bl, 0], kbuf[s, bl, 1]], axis=1)
            sc = lax.dot_general(lhs, k_cat, (((1,), (1,)), ((), ())), preferred_element_type=F32) * scale
            sc_v[bl * 32:(bl + 1) * 32, :] = jnp.where(gap <= ln, sc, -jnp.inf)
        for c in range(BBLK // 2):
            rows = slice(c * 64, (c + 1) * 64)
            sc = sc_v[rows, :]
            ex = jnp.exp(sc - jnp.max(sc, axis=1, keepdims=True))
            ex_v[rows, :] = ex.astype(BF16)
            den_v[rows, :] = jnp.broadcast_to(jnp.sum(ex, axis=1, keepdims=True), (64, HEAD))
        for bl in range(BBLK):
            v_cat = jnp.concatenate([vbuf[s, bl, 0], vbuf[s, bl, 1]], axis=1)
            mix = jnp.dot(ex_v[bl * 32:(bl + 1) * 32, :], v_cat, preferred_element_type=F32)
            o32[bl * 32:bl * 32 + 16, :] = mix[:16, :HEAD] / den_v[bl * 32:bl * 32 + 16, :]
            o32[bl * 32 + 16:bl * 32 + 32, :] = mix[16:, HEAD:] / den_v[bl * 32 + 16:bl * 32 + 32, :]
        for t in range(STEPS):
            for hd in range(Q_LOC):
                row = (hd // GROUP) * 16 + t * GROUP + hd % GROUP
                slab = o32[pl.ds(row, BBLK, stride=32), :]
                o_buf[i % 2, t, :, hd * HEAD:(hd + 1) * HEAD] = slab.astype(BF16)
        for t in range(STEPS):
            o_copy(i, t).start()
        return 0

    lax.fori_loop(0, N_BLK, block, 0)
    for i in range(N_BLK - 2, N_BLK):
        out_copy(i, i % SLOTS, 0).wait()
        out_copy(i, i % SLOTS, 1).wait()
        for t in range(STEPS):
            o_copy(i, t).wait()


def run_attn(lengths, q32, k_new, v_new, k_cache, v_cache):
    return pl.pallas_call(
        attn_kernel,
        out_shape=(jax.ShapeDtypeStruct((STEPS, BATCH, Q_LOC * HEAD), BF16),
                   jax.ShapeDtypeStruct(k_cache.shape, BF16),
                   jax.ShapeDtypeStruct(v_cache.shape, BF16)),
        in_specs=[SM, HB, HB, HB, HB, HB],
        out_specs=(HB, HB, HB),
        scratch_shapes=[
            pltpu.VMEM((SLOTS, BBLK, KV_LOC, SEQ, HEAD), BF16),
            pltpu.VMEM((SLOTS, BBLK, KV_LOC, SEQ, HEAD), BF16),
            pltpu.VMEM((BBLK * 32, HEAD), F32),
            pltpu.VMEM((BBLK * 32, HEAD), F32),
            pltpu.VMEM((BBLK * 32, SEQ), F32),
            pltpu.VMEM((BBLK * 32, SEQ), BF16),
            pltpu.VMEM((BBLK * 32, HEAD), F32),
            pltpu.VMEM((2, STEPS, BBLK, Q_LOC * HEAD), BF16),
            pltpu.VMEM((30, BATCH, HEAD), BF16),
            pltpu.VMEM((ROWS, KV_LOC * HEAD), BF16),
            pltpu.VMEM((ROWS, KV_LOC * HEAD), BF16),
            pltpu.SemaphoreType.DMA((2, SLOTS)),
            pltpu.SemaphoreType.DMA((2, SLOTS)),
            pltpu.SemaphoreType.DMA((2, STEPS)),
            pltpu.SemaphoreType.DMA((3,)),
        ],
        compiler_params=pltpu.CompilerParams(vmem_limit_bytes=67043328),
        name='attend',
    )(lengths, q32, k_new, v_new, k_cache, v_cache)


CHUNKS = (64, 64)
CROWS = tuple(STEPS * n for n in CHUNKS)
PIECES = 5
PW = 512
HALF_T = PIECES
RING = 3
RESID = 6
GW = PW // 2
G_TILES = pl.cdiv(FF_LOC, GW)
G_STREAM = G_TILES - RESID
G_EXTRA = G_STREAM - RESID
PHASES = (('g', G_STREAM), ('d', 2 * PIECES), ('g', G_STREAM), ('d', 2 * PIECES))
WO_PER = D_MODEL // (Q_LOC * HEAD)
WO_SLOTS = pl.cdiv(2 * PIECES, WO_PER)
WO_AHEAD = 4


def mlp_kernel(o_hbm, x_hbm, wo_hbm, w1_hbm, w3_hbm, w2_hbm, ga_hbm, gm_hbm,
               y_hbm,
               o_v, xh0, xh1, u0, ps0, ps1, pr0, pr1, r10, r11, r20, r21, a0, a1, ring, ga_ref, gm_ref,
               in_sem, g_sem, wo_sem, ring_sem, res_sem, out_sem,
               p_send, p_recv, c_send, c_recv, a_send, a_recv):
    me = lax.axis_index('tp')
    core = me % 2
    chip = me // 2
    mate = chip * 2 + (1 - core)
    peer = (1 - chip) * 2 + core
    xh = (xh0, xh1)
    u_v = [u0.at[pl.ds(0, n), :] for n in CROWS]
    p_out, p_in = (ps0, ps1), (pr0, pr1)
    r_v = ((r10, r11), (r20, r21))
    a_v = (a0, a1)
    firsts = (0, CHUNKS[0])
    row0 = (0, CROWS[0])

    barrier = pltpu.get_barrier_semaphore()
    for dev in (mate, peer):
        pl.semaphore_signal(barrier, inc=1, device_id={'tp': dev}, device_id_type=MESH)

    bases = []
    total = 0
    for _, n in PHASES:
        bases.append(total)
        total += n

    def out_col(i):
        k = i // 2
        own = i % 2
        half = own * core + (1 - own) * (1 - core)
        return half * HALF_T + k

    def g_col(i):
        return pl.multiple_of(jnp.minimum(i * GW, FF_LOC - GW), 128)

    def g_tile(s):
        return jnp.where(s < G_EXTRA, G_TILES - G_EXTRA + s, 2 * (s - G_EXTRA))

    def tile_copies(kind, idx, slot, sem):
        if kind == 'd':
            col = pl.multiple_of(out_col(idx) * PW, PW)
            return [pltpu.make_async_copy(w2_hbm.at[:, pl.ds(col, PW)], ring.at[slot, pl.ds(0, FF_LOC), :], sem.at[0])]
        col = g_col(idx)
        return [pltpu.make_async_copy(w1_hbm.at[:, pl.ds(col, GW)], ring.at[slot, :, pl.ds(0, GW)], sem.at[0]),
                pltpu.make_async_copy(w3_hbm.at[:, pl.ds(col, GW)], ring.at[slot, :, pl.ds(GW, GW)], sem.at[1])]

    def stream(ph, s, start):
        kind = PHASES[ph][0]
        slot = (bases[ph] + s) % RING
        idx = g_tile(s) if kind == 'g' else s
        for cp in tile_copies(kind, idx, slot, ring_sem.at[slot]):
            if start:
                cp.start()
            else:
                cp.wait()
        return slot

    def refill(ph, s):
        n = PHASES[ph][1]

        @pl.when(s + RING < n)
        def _():
            stream(ph, s + RING, True)

        if ph + 1 < len(PHASES):
            @pl.when(s + RING >= n)
            def _():
                stream(ph + 1, s + RING - n, True)

    o_copies, x_copies = [], []
    for ch in range(2):
        for t in range(STEPS):
            o_copies.append(pltpu.make_async_copy(
                o_hbm.at[t, pl.ds(firsts[ch], CHUNKS[ch]), :],
                o_v.at[pl.ds(row0[ch] + t * CHUNKS[ch], CHUNKS[ch]), :], in_sem.at[0, ch, t]))
            x_copies.append(pltpu.make_async_copy(
                x_hbm.at[t, pl.ds(firsts[ch], CHUNKS[ch]), :],
                xh[ch].at[pl.ds(t * CHUNKS[ch], CHUNKS[ch]), :], in_sem.at[1, ch, t]))
    g_copies = [pltpu.make_async_copy(ga_hbm, ga_ref, g_sem.at[0]), pltpu.make_async_copy(gm_hbm, gm_ref, g_sem.at[1])]
    for cp in o_copies + g_copies:
        cp.start()
    def wo_copy(i):
        col = pl.multiple_of(out_col(i) * PW, PW)
        rows = pl.ds(pl.multiple_of((i % WO_PER) * (Q_LOC * HEAD), Q_LOC * HEAD), Q_LOC * HEAD)
        return pltpu.make_async_copy(wo_hbm.at[:, pl.ds(col, PW)], ring.at[RING + i // WO_PER, rows, :], wo_sem.at[i])

    def res_copies(r):
        return tile_copies('g', 2 * r + 1, RING + r, res_sem.at[r])

    for i in range(WO_AHEAD):
        wo_copy(i).start()

    def mate_copy(ex, ch, k):
        return pltpu.make_async_remote_copy(
            src_ref=p_out[ch].at[k], dst_ref=p_in[ch].at[k], send_sem=p_send.at[ex, ch, k], recv_sem=p_recv.at[ex, ch, k],
            device_id={'tp': mate}, device_id_type=MESH)

    def peer_copy(ex, ch, k):
        return pltpu.make_async_remote_copy(
            src_ref=a_v[ch].at[core * HALF_T + k], dst_ref=r_v[ex][ch].at[k], send_sem=c_send.at[ex, ch, k], recv_sem=c_recv.at[ex, ch, k],
            device_id={'tp': peer}, device_id_type=MESH)

    def gather_copy(ex, ch, k, half):
        j = half * HALF_T + k
        return pltpu.make_async_remote_copy(
            src_ref=a_v[ch].at[j], dst_ref=a_v[ch].at[j], send_sem=a_send.at[ex, ch, k], recv_sem=a_recv.at[ex, ch, k],
            device_id={'tp': mate}, device_id_type=MESH)

    def pair_sum(ex, ch, k):
        mate_copy(ex, ch, k).wait_recv()
        own = core * HALF_T + k
        a_v[ch][own] = (a_v[ch][own].astype(F32) + p_in[ch][k].astype(F32)).astype(BF16)

    def full_sum(ex, ch, k):
        peer_copy(ex, ch, k).wait()
        own = core * HALF_T + k
        a_v[ch][own] = (a_v[ch][own].astype(F32) + r_v[ex][ch][k].astype(F32)).astype(BF16)
        gather_copy(ex, ch, k, core).start()

    def gather_done(ex, ch):
        def step(k, _):
            gather_copy(ex, ch, k, core).wait_send()
            gather_copy(ex, ch, k, 1 - core).wait_recv()
            mate_copy(ex, ch, k).wait_send()
            return 0
        lax.fori_loop(0, PIECES, step, 0)

    def full_sums(ex, ch):
        def step(k, _):
            full_sum(ex, ch, k)
            return 0
        lax.fori_loop(0, PIECES, step, 0)

    def norm_add(ch, gain_ref):
        def step(b, _):
            rows = pl.ds(pl.multiple_of(b * 16, 16), 16)
            acc = jnp.zeros((16, PW), F32)
            for j in range(2 * PIECES):
                val = a_v[ch][j, rows, :].astype(F32)
                acc = acc + val * val
            fac = lax.rsqrt(jnp.sum(acc, axis=1, keepdims=True) / float(D_MODEL) + NORM_EPS)
            for j in range(D_MODEL // HEAD):
                cols = slice(j * HEAD, (j + 1) * HEAD)
                val = a_v[ch][j * HEAD // PW, rows, j * HEAD % PW:j * HEAD % PW + HEAD].astype(F32)
                base = xh[ch][rows, cols].astype(F32)
                xh[ch][rows, cols] = (base + val * fac * gain_ref[j:j + 1, :].astype(F32)).astype(BF16)
            return 0
        lax.fori_loop(0, CROWS[ch] // 16, step, 0)

    for cp in o_copies + g_copies:
        cp.wait()

    def wo_tile(i):
        rows = pl.ds(pl.multiple_of((i % WO_PER) * (Q_LOC * HEAD), Q_LOC * HEAD), Q_LOC * HEAD)
        return jnp.dot(o_v[...], ring[RING + i // WO_PER, rows, :], preferred_element_type=F32).astype(BF16)

    def wo_pair(k):
        for ch in range(2):
            pair_sum(0, ch, k)
        peer_copy(0, 0, k).start()

    def wo_step(k, _):
        wo_copy(2 * k).wait()
        wo_copy(2 * k + 1).wait()

        @pl.when(2 * k + WO_AHEAD < 2 * PIECES)
        def _():
            wo_copy(2 * k + WO_AHEAD).start()
            wo_copy(2 * k + WO_AHEAD + 1).start()
        res = wo_tile(2 * k)
        for ch in range(2):
            p_out[ch][k] = res[row0[ch]:row0[ch] + CROWS[ch]]
            mate_copy(0, ch, k).start()
        res = wo_tile(2 * k + 1)
        for ch in range(2):
            a_v[ch][core * HALF_T + k] = res[row0[ch]:row0[ch] + CROWS[ch]]

        @pl.when(k >= 1)
        def _():
            wo_pair(k - 1)
        return 0

    pl.semaphore_wait(barrier, 2)
    with jax.named_scope('wo'):
        lax.fori_loop(0, PIECES, wo_step, 0)
        wo_pair(PIECES - 1)

    for cp in x_copies:
        cp.start()
    for n in range(RING):
        stream(0, n, True)
    for r in range(RESID):
        for cp in res_copies(r):
            cp.start()
    for cp in x_copies:
        cp.wait()

    def first_sums(k, _):
        full_sum(0, 0, k)
        peer_copy(0, 1, k).start()
        return 0
    with jax.named_scope('sums_a1'):
        lax.fori_loop(0, PIECES, first_sums, 0)
    with jax.named_scope('gather_a1'):
        gather_done(0, 0)
    with jax.named_scope('norm_a1'):
        norm_add(0, ga_ref)

    def gate_up(ph, ch):
        def tile(i, slot):
            acc = jnp.dot(xh[ch][...], ring[slot], preferred_element_type=F32)
            gate = acc[:, :GW]
            act = (gate * jax.nn.sigmoid(gate)) * acc[:, GW:]
            u_v[ch][:, pl.ds(g_col(i), GW)] = act.astype(BF16)

        def single(q, _):
            tile(g_tile(q), stream(ph, q, False))
            refill(ph, q)
            return 0

        def pair(q, _):
            slot = stream(ph, G_EXTRA + q, False)
            if ph == 0:
                for cp in res_copies(q):
                    cp.wait()
            tile(2 * q, slot)
            tile(2 * q + 1, RING + q)
            refill(ph, G_EXTRA + q)
            return 0
        lax.fori_loop(0, G_EXTRA, single, 0)
        lax.fori_loop(0, RESID, pair, 0)

    def down(ph, ch, also):
        def d_tile(i):
            slot = stream(ph, i, False)
            res = jnp.dot(u_v[ch][...], ring[slot, pl.ds(0, FF_LOC), :], preferred_element_type=F32).astype(BF16)
            refill(ph, i)
            return res

        def step(k, _):
            also(k)
            p_out[ch][k] = d_tile(2 * k)
            mate_copy(1, ch, k).start()

            @pl.when(k >= 1)
            def _():
                pair_sum(1, ch, k - 1)
                peer_copy(1, ch, k - 1).start()
            a_v[ch][core * HALF_T + k] = d_tile(2 * k + 1)
            return 0
        lax.fori_loop(0, PIECES, step, 0)

    def down_last(ch):
        pair_sum(1, ch, PIECES - 1)
        peer_copy(1, ch, PIECES - 1).start()

    with jax.named_scope('gate_up_a'):
        gate_up(0, 0)
    with jax.named_scope('down_a'):
        down(1, 0, lambda k: full_sum(0, 1, k))
    with jax.named_scope('gather_b1'):
        gather_done(0, 1)
    with jax.named_scope('norm_b1'):
        norm_add(1, ga_ref)
        down_last(0)
    with jax.named_scope('gate_up_b'):
        gate_up(2, 1)
    with jax.named_scope('down_b'):
        down(3, 1, lambda k: full_sum(1, 0, k))

    def y_copies(ch):
        return [pltpu.make_async_copy(xh[ch].at[pl.ds(t * CHUNKS[ch], CHUNKS[ch]), :],
                                      y_hbm.at[t, pl.ds(firsts[ch], CHUNKS[ch]), :], out_sem.at[ch, t]) for t in range(STEPS)]

    with jax.named_scope('gather_a2'):
        gather_done(1, 0)
    with jax.named_scope('norm_a2'):
        norm_add(0, gm_ref)
        down_last(1)
    for cp in y_copies(0):
        cp.start()
    with jax.named_scope('sums_b2'):
        full_sums(1, 1)
    with jax.named_scope('gather_b2'):
        gather_done(1, 1)
    with jax.named_scope('norm_b2'):
        norm_add(1, gm_ref)
    for cp in y_copies(1):
        cp.start()
    with jax.named_scope('y_out'):
        for ch in range(2):
            for cp in y_copies(ch):
                cp.wait()


def run_mlp(o, x_seq, w_o, w_gate, w_up, w_down, g_a, g_m):
    piece = lambda ch: pltpu.VMEM((PIECES, CROWS[ch], PW), BF16)
    sem = pltpu.SemaphoreType.DMA
    return pl.pallas_call(
        mlp_kernel,
        out_shape=jax.ShapeDtypeStruct((STEPS, BATCH, D_MODEL), BF16),
        in_specs=[HB] * 8,
        out_specs=HB,
        scratch_shapes=[
            pltpu.VMEM((ROWS, Q_LOC * HEAD), BF16),
            pltpu.VMEM((CROWS[0], D_MODEL), BF16), pltpu.VMEM((CROWS[1], D_MODEL), BF16),
            pltpu.VMEM((max(CROWS), FF_LOC), BF16),
            piece(0), piece(1), piece(0), piece(1),
            piece(0), piece(1), piece(0), piece(1),
            pltpu.VMEM((2 * PIECES, CROWS[0], PW), BF16), pltpu.VMEM((2 * PIECES, CROWS[1], PW), BF16),
            pltpu.VMEM((RING + RESID, D_MODEL, PW), BF16),
            pltpu.VMEM((D_MODEL // HEAD, HEAD), BF16), pltpu.VMEM((D_MODEL // HEAD, HEAD), BF16),
            sem((2, 2, STEPS)), sem((2,)), sem((2 * PIECES,)), sem((RING, 2)), sem((RESID, 2)), sem((2, STEPS)),
            sem((2, 2, PIECES)), sem((2, 2, PIECES)), sem((2, 2, PIECES)),
            sem((2, 2, PIECES)), sem((2, 2, PIECES)), sem((2, 2, PIECES)),
        ],
        compiler_params=pltpu.CompilerParams(collective_id=1, has_side_effects=True, vmem_limit_bytes=67043328),
        name='wo_mlp',
    )(o, x_seq, w_o, w_gate, w_up, w_down, g_a, g_m)


def solution(mesh):
    def local_run(x_seq, cache_len, k_cache, v_cache, w_q, w_k, w_v, w_o, w_gate, w_up, w_down, g_q, g_k, g_attn, g_mlp):
        inv_freq = ROPE_THETA ** (-(np.arange(HEAD // 2, dtype=np.float32) * np.float32(2.0 / HEAD)))
        freq_row = jnp.asarray(np.concatenate([inv_freq, inv_freq])[None, :], dtype=F32)
        tiled = lambda g: g.reshape(-1, HEAD)
        q_rot, k_new, v_new = run_qkv(x_seq.reshape(ROWS, D_MODEL), w_q, w_k, w_v, tiled(g_q), tiled(g_k), cache_len[None, :], freq_row)
        o, k_out, v_out = run_attn(cache_len, q_rot, k_new, v_new, k_cache, v_cache)
        y = run_mlp(o, x_seq, w_o, w_gate, w_up, w_down, tiled(g_attn), tiled(g_mlp))
        return y, k_out, v_out

    data_spec = P(None, 'dp', None)
    cache_spec = P('dp', 'tp', None, None)
    col_spec = P(None, 'tp')
    row_spec = P('tp', None)
    arg_specs = (data_spec, P('dp'), cache_spec, cache_spec, col_spec, col_spec, col_spec, row_spec, col_spec, col_spec, row_spec, P('tp'), P('tp'), P(None), P(None))
    out_specs = (data_spec, cache_spec, cache_spec)
    return jax.shard_map(local_run, mesh=mesh, in_specs=arg_specs, out_specs=out_specs, check_vma=False)
```

```python
import jax
import jax.numpy as jnp
import numpy as np
from jax import lax
from jax.experimental import pallas as pl
from jax.experimental.pallas import tpu as pltpu
from jax.sharding import PartitionSpec as P

ROPE_THETA = 500000.0
NORM_EPS = 1e-6
MESH = pl.DeviceIdType.MESH
F32 = jnp.float32
PAIR = range(2)
VMEM_ALL = 67043328
BF16 = jnp.bfloat16

STEPS = 3
BATCH = 128
ROWS = STEPS * BATCH
D_MODEL = 5120
HEAD = 128
KV_LOC = 2
GROUP = 5
Q_LOC = KV_LOC * GROUP
SEQ = 256
FF_LOC = 3456
KV_W = KV_LOC * HEAD
Q_W = Q_LOC * HEAD

ANY = pl.BlockSpec(memory_space=pl.ANY)
VM = pl.BlockSpec(memory_space=pltpu.VMEM)
SM = pl.BlockSpec(memory_space=pltpu.SMEM)
HB = pl.BlockSpec(memory_space=pltpu.HBM)


N_TILE = 512


def qkv_kernel(x_hbm, wq_hbm, wk_hbm, wv_hbm, gq_hbm, gk_hbm, len_hbm, freq_hbm,
               q_hbm, k_hbm, v_hbm,
               x_v, w_v, raw, cos_v, sin_v, sq_acc, sq_own, sq_recv, q_v, k_v, v_v, gq_v, gk_v, len_v, freq_v,
               x_sem, w_sem, send_sem, recv_sem, t_sem, o_sem):
    me = lax.axis_index('tp')
    barrier = pltpu.get_barrier_semaphore()
    for d in range(1, 4):
        pl.semaphore_signal(barrier, inc=1, device_id={'tp': (me + d) % 4}, device_id_type=MESH)

    half_k = D_MODEL // 2
    halves = [pl.ds(n * half_k, half_k) for n in PAIR]
    x_copies = [pltpu.make_async_copy(x_hbm.at[:, h], x_v.at[:, h], x_sem.at[n]) for n, h in enumerate(halves)]
    w_copies = [
        [pltpu.make_async_copy(wq_hbm.at[h, pl.ds(0, N_TILE)], w_v.at[0, h], w_sem.at[n]) for n, h in enumerate(halves)],
        [pltpu.make_async_copy(wq_hbm.at[:, pl.ds(N_TILE, N_TILE)], w_v.at[1], w_sem.at[2])],
        [pltpu.make_async_copy(wq_hbm.at[:, pl.ds(1024, 256)], w_v.at[2, :, pl.ds(0, 256)], w_sem.at[3]),
         pltpu.make_async_copy(wk_hbm, w_v.at[2, :, pl.ds(256, 256)], w_sem.at[4])],
        [pltpu.make_async_copy(wv_hbm, w_v.at[3, :, pl.ds(0, 256)], w_sem.at[5])],
    ]
    t_copies = [pltpu.make_async_copy(src, dst, t_sem.at[n])
                for n, (src, dst) in enumerate(((len_hbm, len_v), (freq_hbm, freq_v), (gq_hbm, gq_v), (gk_hbm, gk_v)))]
    for cp in t_copies:
        cp.start()
    x_copies[0].start()
    w_copies[0][0].start()

    for cp in t_copies:
        cp.wait()
    len_col = jnp.transpose(jnp.broadcast_to(len_v[...].astype(F32), (HEAD, BATCH)))
    sign = jnp.where(lax.broadcasted_iota(jnp.int32, (BATCH, HEAD), 1) < HEAD // 2, -1.0, 1.0)
    for t in range(STEPS):
        rows = pl.ds(t * BATCH, BATCH)
        ang = (len_col + float(t)) * freq_v[...]
        cos_v[rows, :] = jnp.cos(ang)
        sin_v[rows, :] = jnp.sin(ang) * sign

    x_copies[1].start()
    w_copies[0][1].start()

    def piece(col, rows):
        return raw[col // N_TILE, rows, col % N_TILE:col % N_TILE + HEAD]

    def square(cols, rows, acc):
        for col in cols:
            val = piece(col, rows)
            acc = acc + val * val
        return acc

    all_rows = [pl.ds(t * BATCH, BATCH) for t in range(STEPS)]
    zero = jnp.zeros((BATCH, HEAD), F32)

    half_rows = [pl.ds(n * (ROWS // 2), ROWS // 2) for n in PAIR]

    def tile_dot(i, ks=slice(None)):
        return [jnp.dot(x_v[rows, ks], w_v[i, ks, :], preferred_element_type=F32) for rows in half_rows]

    def keep(i, parts):
        for rows, part in zip(half_rows, parts):
            raw[i, rows, :] = part.astype(BF16).astype(F32)

    x_copies[0].wait()
    w_copies[0][0].wait()
    w_copies[1][0].start()
    for rows, part in zip(half_rows, tile_dot(0, halves[0])):
        raw[0, rows, :] = part
    x_copies[1].wait()
    w_copies[0][1].wait()
    for cp in w_copies[2]:
        cp.start()
    keep(0, [raw[0, rows, :] + part for rows, part in zip(half_rows, tile_dot(0, halves[1]))])
    w_copies[1][0].wait()
    w_copies[3][0].start()
    keep(1, tile_dot(1))
    for cp in w_copies[2]:
        cp.wait()
    for t in range(STEPS):
        sq_acc[all_rows[t], :] = square(range(0, 1024, HEAD), all_rows[t], zero)
    keep(2, tile_dot(2))
    w_copies[3][0].wait()

    first_row = lax.broadcasted_iota(jnp.int32, (8, BATCH), 0) == 0
    for t in range(STEPS):
        rows = all_rows[t]
        sums = [jnp.sum(jnp.transpose(acc), axis=0, keepdims=True)
                for acc in (square(range(1024, 1280, HEAD), rows, sq_acc[rows, :]), square(range(1280, 1536, HEAD), rows, zero))]
        sq_own[:, t * BATCH:(t + 1) * BATCH] = jnp.where(first_row, sums[0], sums[1])

    with jax.named_scope('k1_barrier'):
        pl.semaphore_wait(barrier, 3)
    copies = []
    for d in range(1, 4):
        cp = pltpu.make_async_remote_copy(
            src_ref=sq_own, dst_ref=sq_recv.at[d - 1], send_sem=send_sem.at[d - 1], recv_sem=recv_sem.at[d - 1],
            device_id={'tp': (me + d) % 4}, device_id_type=MESH)
        cp.start()
        copies.append(cp)
    for rows in half_rows:
        v_v[rows, :] = jnp.dot(x_v[rows, :], w_v[3, :, pl.ds(0, 256)], preferred_element_type=F32).astype(BF16)
    outs = [pltpu.make_async_copy(v_v, v_hbm, o_sem.at[0])]
    outs[0].start()
    with jax.named_scope('k1_recv'):
        for cp in copies:
            cp.wait()

    q_width = float(Q_LOC * HEAD * 4)
    k_width = float(KV_LOC * HEAD * 4)
    for t in range(STEPS):
        cols = slice(t * BATCH, (t + 1) * BATCH)
        rows = all_rows[t]
        tot = sq_own[:, cols] + sq_recv[0, :, cols] + sq_recv[1, :, cols] + sq_recv[2, :, cols]
        q_fac = lax.rsqrt(tot[0:1] / q_width + NORM_EPS)
        k_fac = lax.rsqrt(tot[1:2] / k_width + NORM_EPS)
        q_col = jnp.transpose(jnp.broadcast_to(q_fac, (HEAD, BATCH)))
        k_col = jnp.transpose(jnp.broadcast_to(k_fac, (HEAD, BATCH)))
        cos_t = cos_v[rows, :]
        sin_t = sin_v[rows, :]
        for hd in range(Q_LOC):
            val = piece(hd * HEAD, rows) * q_col * gq_v[hd:hd + 1, :].astype(F32)
            rot = val * cos_t + pltpu.roll(val, HEAD // 2, 1) * sin_t
            q_v[(hd // GROUP) * 15 + t * GROUP + hd % GROUP] = rot.astype(BF16)
        for kv in range(KV_LOC):
            val = piece((Q_LOC + kv) * HEAD, rows) * k_col * gk_v[kv:kv + 1, :].astype(F32)
            rot = val * cos_t + pltpu.roll(val, HEAD // 2, 1) * sin_t
            k_v[rows, kv * HEAD:(kv + 1) * HEAD] = rot.astype(BF16)
        for kv in range(KV_LOC):
            slabs = pl.ds(kv * 15 + t * GROUP, GROUP)
            outs.append(pltpu.make_async_copy(q_v.at[slabs], q_hbm.at[slabs], o_sem.at[len(outs)]))
        outs.append(pltpu.make_async_copy(k_v.at[rows], k_hbm.at[rows], o_sem.at[len(outs)]))
        for cp in outs[-3:]:
            cp.start()
    with jax.named_scope('k1_out'):
        for cp in outs:
            cp.wait()


def run_qkv(x2, w_q, w_k, w_v, g_q, g_k, len_row, freq_row):
    return pl.pallas_call(
        qkv_kernel,
        out_shape=(jax.ShapeDtypeStruct((30, BATCH, HEAD), BF16),
                   jax.ShapeDtypeStruct((ROWS, KV_W), BF16),
                   jax.ShapeDtypeStruct((ROWS, KV_W), BF16)),
        in_specs=[HB] * 8,
        out_specs=(HB, HB, HB),
        scratch_shapes=[
            pltpu.VMEM((ROWS, D_MODEL), BF16),
            pltpu.VMEM((4, D_MODEL, N_TILE), BF16),
            pltpu.VMEM((3, ROWS, N_TILE), F32),
            *[pltpu.VMEM((ROWS, HEAD), F32)] * 3,
            pltpu.VMEM((8, ROWS), F32),
            pltpu.VMEM((3, 8, ROWS), F32),
            pltpu.VMEM((30, BATCH, HEAD), BF16),
            pltpu.VMEM((ROWS, KV_W), BF16),
            pltpu.VMEM((ROWS, KV_W), BF16),
            pltpu.VMEM((Q_LOC, HEAD), BF16),
            pltpu.VMEM((KV_LOC, HEAD), BF16),
            pltpu.VMEM((1, BATCH), jnp.int32),
            pltpu.VMEM((1, HEAD), F32),
            *[pltpu.SemaphoreType.DMA((n,)) for n in (2, 6, 3, 3, 4, 10)],
        ],
        compiler_params=pltpu.CompilerParams(collective_id=0, has_side_effects=True, vmem_limit_bytes=VMEM_ALL),
        name='qkv_rope',
    )(x2, w_q, w_k, w_v, g_q, g_k, len_row, freq_row)


BBLK = 16
N_BLK = BATCH // BBLK
SLOTS = 4


def attn_kernel(len_ref, q_hbm, kn_hbm, vn_hbm, kc_hbm, vc_hbm,
                o_hbm, ko_hbm, vo_hbm,
                kbuf, vbuf, q32, o32, sc_v, ex_v, den_v, o_buf, q_ref, kn_ref, vn_ref, in_sem, out_sem, o_sem, t_sem):
    def in_copy(i, s, which):
        src = (kc_hbm, vc_hbm)[which]
        dst = (kbuf, vbuf)[which]
        return pltpu.make_async_copy(src.at[pl.ds(i * BBLK, BBLK)], dst.at[s], in_sem.at[which, s])

    def out_copy(i, s, which):
        dst = (ko_hbm, vo_hbm)[which]
        src = (kbuf, vbuf)[which]
        return pltpu.make_async_copy(src.at[s], dst.at[pl.ds(i * BBLK, BBLK)], out_sem.at[which, s])

    def o_copy(i, t):
        return pltpu.make_async_copy(o_buf.at[i % 2, t], o_hbm.at[t, pl.ds(pl.multiple_of(i * BBLK, BBLK), BBLK), :], o_sem.at[i % 2, t])

    t_copies = [pltpu.make_async_copy(src, dst, t_sem.at[n])
                for n, (src, dst) in enumerate(((kn_hbm, kn_ref), (vn_hbm, vn_ref), (q_hbm, q_ref)))]
    for cp in t_copies:
        cp.start()
    for i in PAIR:
        for which in PAIR:
            in_copy(i, i, which).start()
    for pad in (15, 31):
        q32[pl.ds(pad, BBLK, stride=32), :] = jnp.zeros((BBLK, HEAD), F32)

    scale = HEAD ** -0.5
    row_id = lax.broadcasted_iota(jnp.int32, (32, SEQ), 0)
    col_id = lax.broadcasted_iota(jnp.int32, (32, SEQ), 1)
    sub = row_id - jnp.where(row_id >= 16, 16, 0)
    step_of = jnp.where(sub >= 5, 1, 0) + jnp.where(sub >= 10, 1, 0)
    gap = col_id - step_of
    win_id = lax.broadcasted_iota(jnp.int32, (32, HEAD), 0)

    for cp in t_copies:
        cp.wait()

    def block(i, _):
        s = i % SLOTS

        @pl.when(i >= 2)
        def _():
            for which in PAIR:
                out_copy(i - 2, (i + 2) % SLOTS, which).wait()
            for t in range(STEPS):
                o_copy(i - 2, t).wait()

        @pl.when(i + 2 < N_BLK)
        def _():
            for which in PAIR:
                in_copy(i + 2, (i + 2) % SLOTS, which).start()

        for which in PAIR:
            in_copy(i, s, which).wait()

        news = []
        for src in (kn_ref, vn_ref):
            news.append([src[pl.ds(pl.multiple_of(t * BATCH + i * BBLK, BBLK), BBLK), :].astype(F32) for t in range(STEPS)])
        for bl in range(BBLK):
            ln = len_ref[i * BBLK + bl]
            w0 = jnp.minimum((ln // 16) * 16, SEQ - 32)
            win = pl.ds(pl.multiple_of(w0, 16), 32)
            rel = win_id - (ln - w0)
            for buf, new in ((kbuf, news[0]), (vbuf, news[1])):
                for kv in range(KV_LOC):
                    val = buf[s, bl, kv, win, :].astype(F32)
                    for t in range(STEPS):
                        row = new[t][bl:bl + 1, kv * HEAD:(kv + 1) * HEAD]
                        val = jnp.where(rel == t, jnp.broadcast_to(row, (32, HEAD)), val)
                    buf[s, bl, kv, win, :] = val.astype(BF16)
        for which in PAIR:
            out_copy(i, s, which).start()

        zero_q = jnp.zeros((16, HEAD), BF16)
        for row in range(30):
            q32[pl.ds(row + row // 15, BBLK, stride=32), :] = q_ref[row, pl.ds(pl.multiple_of(i * BBLK, BBLK), BBLK), :].astype(F32)
        for bl in range(BBLK):
            ln = len_ref[i * BBLK + bl]
            q_b = q32[bl * 32:(bl + 1) * 32, :].astype(BF16)
            lhs = jnp.concatenate([jnp.concatenate([q_b[:16], zero_q], axis=1),
                                   jnp.concatenate([zero_q, q_b[16:]], axis=1)], axis=0)
            k_cat = jnp.concatenate([kbuf[s, bl, 0], kbuf[s, bl, 1]], axis=1)
            sc = lax.dot_general(lhs, k_cat, (((1,), (1,)), ((), ())), preferred_element_type=F32) * scale
            sc_v[bl * 32:(bl + 1) * 32, :] = jnp.where(gap <= ln, sc, -jnp.inf)
        for c in range(BBLK // 2):
            rows = slice(c * 64, (c + 1) * 64)
            sc = sc_v[rows, :]
            ex = jnp.exp(sc - jnp.max(sc, axis=1, keepdims=True))
            ex_v[rows, :] = ex.astype(BF16)
            den_v[rows, :] = jnp.broadcast_to(jnp.sum(ex, axis=1, keepdims=True), (64, HEAD))
        for bl in range(BBLK):
            v_cat = jnp.concatenate([vbuf[s, bl, 0], vbuf[s, bl, 1]], axis=1)
            mix = jnp.dot(ex_v[bl * 32:(bl + 1) * 32, :], v_cat, preferred_element_type=F32)
            o32[bl * 32:bl * 32 + 16, :] = mix[:16, :HEAD] / den_v[bl * 32:bl * 32 + 16, :]
            o32[bl * 32 + 16:bl * 32 + 32, :] = mix[16:, HEAD:] / den_v[bl * 32 + 16:bl * 32 + 32, :]
        for t in range(STEPS):
            for hd in range(Q_LOC):
                row = (hd // GROUP) * 16 + t * GROUP + hd % GROUP
                slab = o32[pl.ds(row, BBLK, stride=32), :]
                o_buf[i % 2, t, :, hd * HEAD:(hd + 1) * HEAD] = slab.astype(BF16)
        for t in range(STEPS):
            o_copy(i, t).start()
        return 0

    lax.fori_loop(0, N_BLK, block, 0)
    for i in range(N_BLK - 2, N_BLK):
        for which in PAIR:
            out_copy(i, i % SLOTS, which).wait()
        for t in range(STEPS):
            o_copy(i, t).wait()


def run_attn(lengths, q32, k_new, v_new, k_cache, v_cache):
    return pl.pallas_call(
        attn_kernel,
        out_shape=(jax.ShapeDtypeStruct((STEPS, BATCH, Q_W), BF16),
                   jax.ShapeDtypeStruct(k_cache.shape, BF16),
                   jax.ShapeDtypeStruct(v_cache.shape, BF16)),
        in_specs=[SM, HB, HB, HB, HB, HB],
        out_specs=(HB, HB, HB),
        scratch_shapes=[
            pltpu.VMEM((SLOTS, BBLK, KV_LOC, SEQ, HEAD), BF16),
            pltpu.VMEM((SLOTS, BBLK, KV_LOC, SEQ, HEAD), BF16),
            pltpu.VMEM((BBLK * 32, HEAD), F32),
            pltpu.VMEM((BBLK * 32, HEAD), F32),
            pltpu.VMEM((BBLK * 32, SEQ), F32),
            pltpu.VMEM((BBLK * 32, SEQ), BF16),
            pltpu.VMEM((BBLK * 32, HEAD), F32),
            pltpu.VMEM((2, STEPS, BBLK, Q_W), BF16),
            pltpu.VMEM((30, BATCH, HEAD), BF16),
            pltpu.VMEM((ROWS, KV_W), BF16),
            pltpu.VMEM((ROWS, KV_W), BF16),
            pltpu.SemaphoreType.DMA((2, SLOTS)),
            pltpu.SemaphoreType.DMA((2, SLOTS)),
            pltpu.SemaphoreType.DMA((2, STEPS)),
            pltpu.SemaphoreType.DMA((3,)),
        ],
        compiler_params=pltpu.CompilerParams(vmem_limit_bytes=VMEM_ALL),
        name='attend',
    )(lengths, q32, k_new, v_new, k_cache, v_cache)


CHUNKS = (64, 64)
CROWS = tuple(STEPS * n for n in CHUNKS)
PIECES = 5
PW = 512
D_TILES = PIECES + PIECES
HALF_T = PIECES
RING = 3
RESID = 6
GW = PW // 2
G_TILES = pl.cdiv(FF_LOC, GW)
G_STREAM = G_TILES - RESID
G_EXTRA = G_STREAM - RESID
PHASES = (('g', G_STREAM), ('d', D_TILES), ('g', G_STREAM), ('d', D_TILES))
WO_PER = D_MODEL // Q_W
WO_SLOTS = pl.cdiv(D_TILES, WO_PER)
WO_AHEAD = 2
B_LAG = 2
WHOLE = 2
TAIL_ROWS = ((0, 2 * CHUNKS[1]), (2 * CHUNKS[1], CHUNKS[1]))


def mlp_kernel(o_hbm, x_hbm, wo_hbm, w1_hbm, w3_hbm, w2_hbm, ga_hbm, gm_hbm,
               y_hbm,
               o_v, xh0, xh1, u0, ps0, ps1, pr0, pr1, r10, r11, r20, r21, a0, a1, ring, ga_ref, gm_ref,
               in_sem, g_sem, wo_sem, ring_sem, res_sem, out_sem,
               p_send, p_recv, c_send, c_recv, a_send, a_recv, t_send, t_recv):
    me = lax.axis_index('tp')
    core = me % 2
    chip = me // 2
    mate = chip * 2 + (1 - core)
    peer = (1 - chip) * 2 + core
    xh = (xh0, xh1)
    u_v = [u0.at[pl.ds(0, n), :] for n in CROWS]
    p_out, p_in = (ps0, ps1), (pr0, pr1)
    r_v = ((r10, r11), (r20, r21))
    a_v = (a0, a1)
    firsts = (0, CHUNKS[0])
    row0 = (0, CROWS[0])

    barrier = pltpu.get_barrier_semaphore()
    for dev in (mate, peer):
        pl.semaphore_signal(barrier, inc=1, device_id={'tp': dev}, device_id_type=MESH)

    bases = []
    total = 0
    for _, n in PHASES:
        bases.append(total)
        total += n

    def out_col(i):
        k = i // 2
        own = i % 2
        half = own * core + (1 - own) * (1 - core)
        return half * HALF_T + k

    def g_col(i):
        return pl.multiple_of(jnp.minimum(i * GW, FF_LOC - GW), 128)

    def g_tile(s):
        return jnp.where(s < G_EXTRA, G_TILES - G_EXTRA + s, 2 * (s - G_EXTRA))

    def tile_copies(kind, idx, slot, sem):
        if kind == 'd':
            col = pl.multiple_of(out_col(idx) * PW, PW)
            return [pltpu.make_async_copy(w2_hbm.at[:, pl.ds(col, PW)], ring.at[slot, pl.ds(0, FF_LOC), :], sem.at[0])]
        col = g_col(idx)
        return [pltpu.make_async_copy(w1_hbm.at[:, pl.ds(col, GW)], ring.at[slot, :, pl.ds(0, GW)], sem.at[0]),
                pltpu.make_async_copy(w3_hbm.at[:, pl.ds(col, GW)], ring.at[slot, :, pl.ds(GW, GW)], sem.at[1])]

    def stream(ph, s, start):
        kind = PHASES[ph][0]
        slot = (bases[ph] + s) % RING
        idx = g_tile(s) if kind == 'g' else s
        for cp in tile_copies(kind, idx, slot, ring_sem.at[slot]):
            if start:
                cp.start()
            else:
                cp.wait()
        return slot

    def refill(ph, s):
        n = PHASES[ph][1]

        @pl.when(s + RING < n)
        def _():
            stream(ph, s + RING, True)

        if ph + 1 < len(PHASES):
            @pl.when(s + RING >= n)
            def _():
                stream(ph + 1, s + RING - n, True)

    o_copies, x_copies = [], []
    for ch in PAIR:
        for t in range(STEPS):
            o_copies.append(pltpu.make_async_copy(
                o_hbm.at[t, pl.ds(firsts[ch], CHUNKS[ch]), :],
                o_v.at[pl.ds(row0[ch] + t * CHUNKS[ch], CHUNKS[ch]), :], in_sem.at[0, ch, t]))
            x_copies.append(pltpu.make_async_copy(
                x_hbm.at[t, pl.ds(firsts[ch], CHUNKS[ch]), :],
                xh[ch].at[pl.ds(t * CHUNKS[ch], CHUNKS[ch]), :], in_sem.at[1, ch, t]))
    g_copies = [pltpu.make_async_copy(ga_hbm, ga_ref, g_sem.at[0]), pltpu.make_async_copy(gm_hbm, gm_ref, g_sem.at[1])]
    for cp in o_copies + g_copies:
        cp.start()
    def wo_copy(i):
        col = pl.multiple_of(out_col(i) * PW, PW)
        rows = pl.ds(pl.multiple_of((i % WO_PER) * Q_W, Q_W), Q_W)
        return pltpu.make_async_copy(wo_hbm.at[:, pl.ds(col, PW)], ring.at[RING + i // WO_PER, rows, :], wo_sem.at[i])

    def res_copies(r):
        return tile_copies('g', 2 * r + 1, RING + r, res_sem.at[r])

    for i in range(WO_AHEAD):
        wo_copy(i).start()

    def mate_copy(ex, ch, k):
        return pltpu.make_async_remote_copy(
            src_ref=p_out[ch].at[k], dst_ref=p_in[ch].at[k], send_sem=p_send.at[ex, ch, k], recv_sem=p_recv.at[ex, ch, k],
            device_id={'tp': mate}, device_id_type=MESH)

    def peer_copy(ex, ch, k):
        return pltpu.make_async_remote_copy(
            src_ref=a_v[ch].at[core * HALF_T + k], dst_ref=r_v[ex][ch].at[k], send_sem=c_send.at[ex, ch, k], recv_sem=c_recv.at[ex, ch, k],
            device_id={'tp': peer}, device_id_type=MESH)

    def gather_copy(ex, ch, k, half):
        j = half * HALF_T + k
        return pltpu.make_async_remote_copy(
            src_ref=a_v[ch].at[j], dst_ref=a_v[ch].at[j], send_sem=a_send.at[ex, ch, k], recv_sem=a_recv.at[ex, ch, k],
            device_id={'tp': mate}, device_id_type=MESH)

    def tail_peer(g, k):
        rows = pl.ds(*TAIL_ROWS[g])
        return pltpu.make_async_remote_copy(
            src_ref=a_v[1].at[core * HALF_T + k, rows], dst_ref=r_v[1][1].at[k, rows],
            send_sem=t_send.at[0, g, k - WHOLE], recv_sem=t_recv.at[0, g, k - WHOLE],
            device_id={'tp': peer}, device_id_type=MESH)

    def tail_gather(g, k, half):
        rows = pl.ds(*TAIL_ROWS[g])
        j = half * HALF_T + k
        return pltpu.make_async_remote_copy(
            src_ref=a_v[1].at[j, rows], dst_ref=a_v[1].at[j, rows],
            send_sem=t_send.at[1, g, k - WHOLE], recv_sem=t_recv.at[1, g, k - WHOLE],
            device_id={'tp': mate}, device_id_type=MESH)

    def pair_sum(ex, ch, k):
        mate_copy(ex, ch, k).wait_recv()
        own = core * HALF_T + k
        a_v[ch][own] = (a_v[ch][own].astype(F32) + p_in[ch][k].astype(F32)).astype(BF16)

    def full_sum(ex, ch, k):
        peer_copy(ex, ch, k).wait()
        own = core * HALF_T + k
        a_v[ch][own] = (a_v[ch][own].astype(F32) + r_v[ex][ch][k].astype(F32)).astype(BF16)
        gather_copy(ex, ch, k, core).start()

    def gather_done(ex, ch):
        def step(k, _):
            gather_copy(ex, ch, k, core).wait_send()
            gather_copy(ex, ch, k, 1 - core).wait_recv()
            mate_copy(ex, ch, k).wait_send()
            return 0
        lax.fori_loop(0, PIECES, step, 0)

    def full_sums(ex, ch):
        def step(k, _):
            full_sum(ex, ch, k)
            return 0
        lax.fori_loop(0, PIECES, step, 0)

    def norm_add(ch, gain_ref, then=None, steps=range(STEPS)):
        def step(b, _):
            rows = pl.ds(pl.multiple_of(b * 16, 16), 16)
            acc = jnp.zeros((16, PW), F32)
            for j in range(D_TILES):
                val = a_v[ch][j, rows, :].astype(F32)
                acc = acc + val * val
            fac = lax.rsqrt(jnp.sum(acc, axis=1, keepdims=True) / float(D_MODEL) + NORM_EPS)
            for j in range(D_MODEL // HEAD):
                cols = slice(j * HEAD, (j + 1) * HEAD)
                val = a_v[ch][j * HEAD // PW, rows, j * HEAD % PW:j * HEAD % PW + HEAD].astype(F32)
                base = xh[ch][rows, cols].astype(F32)
                xh[ch][rows, cols] = (base + val * fac * gain_ref[j:j + 1, :].astype(F32)).astype(BF16)
            return 0
        for t in steps:
            lax.fori_loop(t * CHUNKS[ch] // 16, (t + 1) * CHUNKS[ch] // 16, step, 0)
            if then is not None:
                then(t)

    for cp in o_copies + g_copies:
        cp.wait()

    def wo_tile(i, ch):
        rows = pl.ds(pl.multiple_of((i % WO_PER) * Q_W, Q_W), Q_W)
        return jnp.dot(o_v[pl.ds(row0[ch], CROWS[ch]), :], ring[RING + i // WO_PER, rows, :],
                       preferred_element_type=F32).astype(BF16)

    def wo_sweep(ch):
        def step(k, _):
            if ch == 0:
                wo_copy(2 * k).wait()
                wo_copy(2 * k + 1).wait()

                @pl.when(2 * k + WO_AHEAD < D_TILES)
                def _():
                    wo_copy(2 * k + WO_AHEAD).start()
                    wo_copy(2 * k + WO_AHEAD + 1).start()
            p_out[ch][k] = wo_tile(2 * k, ch)
            mate_copy(0, ch, k).start()
            a_v[ch][core * HALF_T + k] = wo_tile(2 * k + 1, ch)

            pair_sum(0, ch, k)
            if ch == 0:
                peer_copy(0, ch, k).start()
            return 0
        lax.fori_loop(0, PIECES, step, 0)

    pl.semaphore_wait(barrier, 2)
    with jax.named_scope('wo'):
        wo_sweep(0)
        for cp in x_copies:
            cp.start()
        for n in range(RING):
            stream(0, n, True)
        for r in range(WO_SLOTS, RESID):
            for cp in res_copies(r):
                cp.start()
        wo_sweep(1)

    for r in range(WO_SLOTS):
        for cp in res_copies(r):
            cp.start()
    with jax.named_scope('sums_a1'):
        def first_sums(k, _):
            full_sum(0, 0, k)

            @pl.when(k >= B_LAG)
            def _():
                peer_copy(0, 1, k - B_LAG).start()
            return 0
        lax.fori_loop(0, PIECES, first_sums, 0)
        for k in range(PIECES - B_LAG, PIECES):
            peer_copy(0, 1, k).start()
    with jax.named_scope('gather_a1'):
        gather_done(0, 0)
    for cp in x_copies:
        cp.wait()
    with jax.named_scope('norm_a1'):
        norm_add(0, ga_ref)

    def gate_up(ph, ch):
        def tile(i, slot):
            acc = jnp.dot(xh[ch][...], ring[slot], preferred_element_type=F32)
            gate = acc[:, :GW]
            act = (gate * jax.nn.sigmoid(gate)) * acc[:, GW:]
            u_v[ch][:, pl.ds(g_col(i), GW)] = act.astype(BF16)

        def single(q, _):
            tile(g_tile(q), stream(ph, q, False))
            refill(ph, q)
            return 0

        def pair(q, _):
            slot = stream(ph, G_EXTRA + q, False)
            if ph == 0:
                for cp in res_copies(q):
                    cp.wait()
            tile(2 * q, slot)
            tile(2 * q + 1, RING + q)
            refill(ph, G_EXTRA + q)
            return 0
        lax.fori_loop(0, G_EXTRA, single, 0)
        lax.fori_loop(0, RESID, pair, 0)

    def down(ph, ch, also, lag):
        def swap(k):
            pair_sum(1, ch, k)
            peer_copy(1, ch, k).start()

        def d_tile(i):
            slot = stream(ph, i, False)
            res = jnp.dot(u_v[ch][...], ring[slot, pl.ds(0, FF_LOC), :], preferred_element_type=F32).astype(BF16)
            refill(ph, i)
            return res

        def step(k, _):
            also(k)
            p_out[ch][k] = d_tile(2 * k)
            mate_copy(1, ch, k).start()

            if lag:
                @pl.when(k >= 1)
                def _():
                    swap(k - 1)
            a_v[ch][core * HALF_T + k] = d_tile(2 * k + 1)
            if not lag:
                pair_sum(1, ch, k)

                @pl.when(k < WHOLE)
                def _():
                    peer_copy(1, ch, k).start()
            return 0
        lax.fori_loop(0, PIECES, step, 0)


    with jax.named_scope('gate_up_a'):
        gate_up(0, 0)
    with jax.named_scope('down_a'):
        down(1, 0, lambda k: full_sum(0, 1, k), True)
    with jax.named_scope('gather_b1'):
        gather_done(0, 1)
    with jax.named_scope('norm_b1'):
        norm_add(1, ga_ref)
        pair_sum(1, 0, PIECES - 1)
        peer_copy(1, 0, PIECES - 1).start()
    with jax.named_scope('gate_up_b'):
        gate_up(2, 1)
    with jax.named_scope('down_b'):
        down(3, 1, lambda k: full_sum(1, 0, k), False)
        for g in PAIR:
            for k in range(WHOLE, PIECES):
                tail_peer(g, k).start()

    def y_copies(ch):
        return [pltpu.make_async_copy(xh[ch].at[pl.ds(t * CHUNKS[ch], CHUNKS[ch]), :],
                                      y_hbm.at[t, pl.ds(firsts[ch], CHUNKS[ch]), :], out_sem.at[ch, t]) for t in range(STEPS)]

    with jax.named_scope('gather_a2'):
        gather_done(1, 0)
    with jax.named_scope('norm_a2'):
        norm_add(0, gm_ref, lambda t: y_copies(0)[t].start())
    with jax.named_scope('sums_b2'):
        def whole_sums(k, _):
            full_sum(1, 1, k)
            return 0
        lax.fori_loop(0, WHOLE, whole_sums, 0)
    for g in PAIR:
        rows = pl.ds(*TAIL_ROWS[g])
        with jax.named_scope(f'sums_b2#g={g}'):
            for k in range(WHOLE, PIECES):
                own = core * HALF_T + k
                tail_peer(g, k).wait()
                a_v[1][own, rows, :] = (a_v[1][own, rows, :].astype(F32) + r_v[1][1][k, rows, :].astype(F32)).astype(BF16)
                tail_gather(g, k, core).start()
        with jax.named_scope(f'gather_b2#g={g}'):
            if g == 0:
                def whole_done(k, _):
                    gather_copy(1, 1, k, core).wait_send()
                    gather_copy(1, 1, k, 1 - core).wait_recv()
                    return 0
                lax.fori_loop(0, WHOLE, whole_done, 0)

                def sends_done(k, _):
                    mate_copy(1, 1, k).wait_send()
                    return 0
                lax.fori_loop(0, PIECES, sends_done, 0)
            for k in range(WHOLE, PIECES):
                tail_gather(g, k, core).wait_send()
                tail_gather(g, k, 1 - core).wait_recv()
        with jax.named_scope(f'norm_b2#g={g}'):
            norm_add(1, gm_ref, lambda t: y_copies(1)[t].start(), ((0, 1), (2,))[g])
    with jax.named_scope('y_out'):
        for ch in PAIR:
            for cp in y_copies(ch):
                cp.wait()


def run_mlp(o, x_seq, w_o, w_gate, w_up, w_down, g_a, g_m):
    sem = pltpu.SemaphoreType.DMA
    return pl.pallas_call(
        mlp_kernel,
        out_shape=jax.ShapeDtypeStruct((STEPS, BATCH, D_MODEL), BF16),
        in_specs=[HB] * 8,
        out_specs=HB,
        scratch_shapes=[
            pltpu.VMEM((ROWS, Q_W), BF16),
            *[pltpu.VMEM((n, D_MODEL), BF16) for n in CROWS],
            pltpu.VMEM((max(CROWS), FF_LOC), BF16),
            *[pltpu.VMEM((PIECES, n, PW), BF16) for n in CROWS * 4],
            *[pltpu.VMEM((D_TILES, n, PW), BF16) for n in CROWS],
            pltpu.VMEM((RING + RESID, D_MODEL, PW), BF16),
            *[pltpu.VMEM((D_MODEL // HEAD, HEAD), BF16)] * 2,
            sem((2, 2, STEPS)), sem((2,)), sem((D_TILES,)), sem((RING, 2)), sem((RESID, 2)), sem((2, STEPS)),
            *[sem((2, 2, PIECES))] * 6,
            *[sem((2, 2, PIECES - WHOLE))] * 2,
        ],
        compiler_params=pltpu.CompilerParams(collective_id=1, has_side_effects=True, vmem_limit_bytes=VMEM_ALL),
        name='wo_mlp',
    )(o, x_seq, w_o, w_gate, w_up, w_down, g_a, g_m)


def solution(mesh):
    def local_run(x_seq, cache_len, k_cache, v_cache, w_q, w_k, w_v, w_o, w_gate, w_up, w_down, g_q, g_k, g_attn, g_mlp):
        inv_freq = ROPE_THETA ** (-(np.arange(HEAD // 2, dtype=np.float32) * np.float32(2.0 / HEAD)))
        freq_row = jnp.asarray(np.concatenate([inv_freq, inv_freq])[None, :], dtype=F32)
        tiled = lambda g: g.reshape(-1, HEAD)
        q_rot, k_new, v_new = run_qkv(x_seq.reshape(ROWS, D_MODEL), w_q, w_k, w_v, tiled(g_q), tiled(g_k), cache_len[None, :], freq_row)
        o, k_out, v_out = run_attn(cache_len, q_rot, k_new, v_new, k_cache, v_cache)
        y = run_mlp(o, x_seq, w_o, w_gate, w_up, w_down, tiled(g_attn), tiled(g_mlp))
        return y, k_out, v_out

    data_spec = P(None, 'dp', None)
    cache_spec = P('dp', 'tp', None, None)
    col_spec = P(None, 'tp')
    row_spec = P('tp', None)
    arg_specs = (data_spec, P('dp'), cache_spec, cache_spec, col_spec, col_spec, col_spec, row_spec, col_spec, col_spec, row_spec, P('tp'), P('tp'), P(None), P(None))
    out_specs = (data_spec, cache_spec, cache_spec)
    return jax.shard_map(local_run, mesh=mesh, in_specs=arg_specs, out_specs=out_specs, check_vma=False)
```

```python
import jax
import jax.numpy as jnp
import numpy as np
from jax import lax
from jax.experimental import pallas as pl
from jax.experimental.pallas import tpu as pltpu
from jax.sharding import PartitionSpec as P

ROPE_THETA = 500000.0
NORM_EPS = 1e-6
MESH = pl.DeviceIdType.MESH
F32 = jnp.float32
PAIR = range(2)
VMEM_ALL = 67043328
BF16 = jnp.bfloat16

STEPS = 3
BATCH = 128
ROWS = STEPS * BATCH
D_MODEL = 5120
HEAD = 128
KV_LOC = 2
GROUP = 5
Q_LOC = KV_LOC * GROUP
SEQ = 256
FF_LOC = 3456
KV_W = KV_LOC * HEAD
Q_W = Q_LOC * HEAD

ANY = pl.BlockSpec(memory_space=pl.ANY)
VM = pl.BlockSpec(memory_space=pltpu.VMEM)
SM = pl.BlockSpec(memory_space=pltpu.SMEM)
HB = pl.BlockSpec(memory_space=pltpu.HBM)


def loop(stop, body, start=0):
    def step(i, carry):
        body(i, carry)
        return carry
    lax.fori_loop(start, stop, step, 0)


N_TILE = 512


def qkv_kernel(x_hbm, wq_hbm, wk_hbm, wv_hbm, gq_hbm, gk_hbm, len_hbm, freq_hbm,
               q_hbm, k_hbm, v_hbm,
               x_v, w_v, raw, cos_v, sin_v, sq_acc, sq_own, sq_recv, q_v, k_v, v_v, gq_v, gk_v, len_v, freq_v,
               x_sem, w_sem, send_sem, recv_sem, t_sem, o_sem):
    me = lax.axis_index('tp')
    barrier = pltpu.get_barrier_semaphore()
    for d in range(1, 4):
        pl.semaphore_signal(barrier, inc=1, device_id={'tp': (me + d) % 4}, device_id_type=MESH)

    half_k = D_MODEL // 2
    halves = [pl.ds(n * half_k, half_k) for n in PAIR]
    x_copies = [pltpu.make_async_copy(x_hbm.at[:, h], x_v.at[:, h], x_sem.at[n]) for n, h in enumerate(halves)]
    w_copies = [
        [pltpu.make_async_copy(wq_hbm.at[h, pl.ds(0, N_TILE)], w_v.at[0, h], w_sem.at[n]) for n, h in enumerate(halves)],
        [pltpu.make_async_copy(wq_hbm.at[:, pl.ds(N_TILE, N_TILE)], w_v.at[1], w_sem.at[2])],
        [pltpu.make_async_copy(wq_hbm.at[:, pl.ds(1024, 256)], w_v.at[2, :, pl.ds(0, 256)], w_sem.at[3]),
         pltpu.make_async_copy(wk_hbm, w_v.at[2, :, pl.ds(256, 256)], w_sem.at[4])],
        [pltpu.make_async_copy(wv_hbm, w_v.at[3, :, pl.ds(0, 256)], w_sem.at[5])],
    ]
    t_copies = [pltpu.make_async_copy(src, dst, t_sem.at[n])
                for n, (src, dst) in enumerate(((len_hbm, len_v), (freq_hbm, freq_v), (gq_hbm, gq_v), (gk_hbm, gk_v)))]
    for cp in t_copies:
        cp.start()
    x_copies[0].start()
    w_copies[0][0].start()

    for cp in t_copies:
        cp.wait()
    len_col = jnp.transpose(jnp.broadcast_to(len_v[...].astype(F32), (HEAD, BATCH)))
    sign = jnp.where(lax.broadcasted_iota(jnp.int32, (BATCH, HEAD), 1) < HEAD // 2, -1.0, 1.0)
    for t in range(STEPS):
        rows = pl.ds(t * BATCH, BATCH)
        ang = (len_col + float(t)) * freq_v[...]
        cos_v[rows, :] = jnp.cos(ang)
        sin_v[rows, :] = jnp.sin(ang) * sign

    x_copies[1].start()
    w_copies[0][1].start()

    def piece(col, rows):
        return raw[col // N_TILE, rows, col % N_TILE:col % N_TILE + HEAD]

    def square(cols, rows, acc):
        for col in cols:
            val = piece(col, rows)
            acc = acc + val * val
        return acc

    all_rows = [pl.ds(t * BATCH, BATCH) for t in range(STEPS)]
    zero = jnp.zeros((BATCH, HEAD), F32)

    half_rows = [pl.ds(n * (ROWS // 2), ROWS // 2) for n in PAIR]

    def tile_dot(i, ks=slice(None)):
        return [jnp.dot(x_v[rows, ks], w_v[i, ks, :], preferred_element_type=F32) for rows in half_rows]

    def keep(i, parts):
        for rows, part in zip(half_rows, parts):
            raw[i, rows, :] = part.astype(BF16).astype(F32)

    x_copies[0].wait()
    w_copies[0][0].wait()
    w_copies[1][0].start()
    for rows, part in zip(half_rows, tile_dot(0, halves[0])):
        raw[0, rows, :] = part
    x_copies[1].wait()
    w_copies[0][1].wait()
    for cp in w_copies[2]:
        cp.start()
    keep(0, [raw[0, rows, :] + part for rows, part in zip(half_rows, tile_dot(0, halves[1]))])
    w_copies[1][0].wait()
    w_copies[3][0].start()
    keep(1, tile_dot(1))
    for cp in w_copies[2]:
        cp.wait()
    for t in range(STEPS):
        sq_acc[all_rows[t], :] = square(range(0, 1024, HEAD), all_rows[t], zero)
    keep(2, tile_dot(2))
    w_copies[3][0].wait()

    first_row = lax.broadcasted_iota(jnp.int32, (8, BATCH), 0) == 0
    for t in range(STEPS):
        rows = all_rows[t]
        sums = [jnp.sum(jnp.transpose(acc), axis=0, keepdims=True)
                for acc in (square(range(1024, 1280, HEAD), rows, sq_acc[rows, :]), square(range(1280, 1536, HEAD), rows, zero))]
        sq_own[:, t * BATCH:(t + 1) * BATCH] = jnp.where(first_row, sums[0], sums[1])

    with jax.named_scope('k1_barrier'):
        pl.semaphore_wait(barrier, 3)
    copies = []
    for d in range(1, 4):
        cp = pltpu.make_async_remote_copy(
            src_ref=sq_own, dst_ref=sq_recv.at[d - 1], send_sem=send_sem.at[d - 1], recv_sem=recv_sem.at[d - 1],
            device_id={'tp': (me + d) % 4}, device_id_type=MESH)
        cp.start()
        copies.append(cp)
    for rows in half_rows:
        v_v[rows, :] = jnp.dot(x_v[rows, :], w_v[3, :, pl.ds(0, 256)], preferred_element_type=F32).astype(BF16)
    outs = [pltpu.make_async_copy(v_v, v_hbm, o_sem.at[0])]
    outs[0].start()
    with jax.named_scope('k1_recv'):
        for cp in copies:
            cp.wait()

    q_width = float(Q_LOC * HEAD * 4)
    k_width = float(KV_LOC * HEAD * 4)
    for t in range(STEPS):
        cols = slice(t * BATCH, (t + 1) * BATCH)
        rows = all_rows[t]
        tot = sq_own[:, cols] + sq_recv[0, :, cols] + sq_recv[1, :, cols] + sq_recv[2, :, cols]
        q_fac = lax.rsqrt(tot[0:1] / q_width + NORM_EPS)
        k_fac = lax.rsqrt(tot[1:2] / k_width + NORM_EPS)
        q_col = jnp.transpose(jnp.broadcast_to(q_fac, (HEAD, BATCH)))
        k_col = jnp.transpose(jnp.broadcast_to(k_fac, (HEAD, BATCH)))
        cos_t = cos_v[rows, :]
        sin_t = sin_v[rows, :]
        for hd in range(Q_LOC):
            val = piece(hd * HEAD, rows) * q_col * gq_v[hd:hd + 1, :].astype(F32)
            rot = val * cos_t + pltpu.roll(val, HEAD // 2, 1) * sin_t
            q_v[(hd // GROUP) * 15 + t * GROUP + hd % GROUP] = rot.astype(BF16)
        for kv in range(KV_LOC):
            val = piece((Q_LOC + kv) * HEAD, rows) * k_col * gk_v[kv:kv + 1, :].astype(F32)
            rot = val * cos_t + pltpu.roll(val, HEAD // 2, 1) * sin_t
            k_v[rows, kv * HEAD:(kv + 1) * HEAD] = rot.astype(BF16)
        for kv in range(KV_LOC):
            slabs = pl.ds(kv * 15 + t * GROUP, GROUP)
            outs.append(pltpu.make_async_copy(q_v.at[slabs], q_hbm.at[slabs], o_sem.at[len(outs)]))
        outs.append(pltpu.make_async_copy(k_v.at[rows], k_hbm.at[rows], o_sem.at[len(outs)]))
        for cp in outs[-3:]:
            cp.start()
    with jax.named_scope('k1_out'):
        for cp in outs:
            cp.wait()


def run_qkv(x2, w_q, w_k, w_v, g_q, g_k, len_row, freq_row):
    return pl.pallas_call(
        qkv_kernel,
        out_shape=(jax.ShapeDtypeStruct((30, BATCH, HEAD), BF16),
                   jax.ShapeDtypeStruct((ROWS, KV_W), BF16),
                   jax.ShapeDtypeStruct((ROWS, KV_W), BF16)),
        in_specs=[HB] * 8,
        out_specs=(HB, HB, HB),
        scratch_shapes=[
            pltpu.VMEM((ROWS, D_MODEL), BF16),
            pltpu.VMEM((4, D_MODEL, N_TILE), BF16),
            pltpu.VMEM((3, ROWS, N_TILE), F32),
            *[pltpu.VMEM((ROWS, HEAD), F32)] * 3,
            pltpu.VMEM((8, ROWS), F32),
            pltpu.VMEM((3, 8, ROWS), F32),
            pltpu.VMEM((30, BATCH, HEAD), BF16),
            pltpu.VMEM((ROWS, KV_W), BF16),
            pltpu.VMEM((ROWS, KV_W), BF16),
            pltpu.VMEM((Q_LOC, HEAD), BF16),
            pltpu.VMEM((KV_LOC, HEAD), BF16),
            pltpu.VMEM((1, BATCH), jnp.int32),
            pltpu.VMEM((1, HEAD), F32),
            *[pltpu.SemaphoreType.DMA((n,)) for n in (2, 6, 3, 3, 4, 10)],
        ],
        compiler_params=pltpu.CompilerParams(collective_id=0, has_side_effects=True, vmem_limit_bytes=VMEM_ALL),
        name='qkv_rope',
    )(x2, w_q, w_k, w_v, g_q, g_k, len_row, freq_row)


BBLK = 16
N_BLK = BATCH // BBLK
SLOTS = 4


def attn_kernel(len_ref, q_hbm, kn_hbm, vn_hbm, kc_hbm, vc_hbm,
                o_hbm, ko_hbm, vo_hbm,
                kbuf, vbuf, q32, o32, sc_v, ex_v, den_v, o_buf, q_ref, kn_ref, vn_ref, in_sem, out_sem, o_sem, t_sem):
    def in_copy(i, s, which):
        src = (kc_hbm, vc_hbm)[which]
        dst = (kbuf, vbuf)[which]
        return pltpu.make_async_copy(src.at[pl.ds(i * BBLK, BBLK)], dst.at[s], in_sem.at[which, s])

    def out_copy(i, s, which):
        dst = (ko_hbm, vo_hbm)[which]
        src = (kbuf, vbuf)[which]
        return pltpu.make_async_copy(src.at[s], dst.at[pl.ds(i * BBLK, BBLK)], out_sem.at[which, s])

    def o_copy(i, t):
        return pltpu.make_async_copy(o_buf.at[i % 2, t], o_hbm.at[t, pl.ds(pl.multiple_of(i * BBLK, BBLK), BBLK), :], o_sem.at[i % 2, t])

    t_copies = [pltpu.make_async_copy(src, dst, t_sem.at[n])
                for n, (src, dst) in enumerate(((kn_hbm, kn_ref), (vn_hbm, vn_ref), (q_hbm, q_ref)))]
    for cp in t_copies:
        cp.start()
    for i in PAIR:
        for which in PAIR:
            in_copy(i, i, which).start()
    for pad in (15, 31):
        q32[pl.ds(pad, BBLK, stride=32), :] = jnp.zeros((BBLK, HEAD), F32)

    scale = HEAD ** -0.5
    row_id = lax.broadcasted_iota(jnp.int32, (32, SEQ), 0)
    col_id = lax.broadcasted_iota(jnp.int32, (32, SEQ), 1)
    sub = row_id - jnp.where(row_id >= 16, 16, 0)
    step_of = jnp.where(sub >= 5, 1, 0) + jnp.where(sub >= 10, 1, 0)
    gap = col_id - step_of
    win_id = lax.broadcasted_iota(jnp.int32, (32, HEAD), 0)

    for cp in t_copies:
        cp.wait()

    def block(i, _):
        s = i % SLOTS

        @pl.when(i >= 2)
        def _():
            for which in PAIR:
                out_copy(i - 2, (i + 2) % SLOTS, which).wait()
            for t in range(STEPS):
                o_copy(i - 2, t).wait()

        @pl.when(i + 2 < N_BLK)
        def _():
            for which in PAIR:
                in_copy(i + 2, (i + 2) % SLOTS, which).start()

        for which in PAIR:
            in_copy(i, s, which).wait()

        news = []
        for src in (kn_ref, vn_ref):
            news.append([src[pl.ds(pl.multiple_of(t * BATCH + i * BBLK, BBLK), BBLK), :].astype(F32) for t in range(STEPS)])
        for bl in range(BBLK):
            ln = len_ref[i * BBLK + bl]
            w0 = jnp.minimum((ln // 16) * 16, SEQ - 32)
            win = pl.ds(pl.multiple_of(w0, 16), 32)
            rel = win_id - (ln - w0)
            for buf, new in ((kbuf, news[0]), (vbuf, news[1])):
                for kv in range(KV_LOC):
                    val = buf[s, bl, kv, win, :].astype(F32)
                    for t in range(STEPS):
                        row = new[t][bl:bl + 1, kv * HEAD:(kv + 1) * HEAD]
                        val = jnp.where(rel == t, jnp.broadcast_to(row, (32, HEAD)), val)
                    buf[s, bl, kv, win, :] = val.astype(BF16)
        for which in PAIR:
            out_copy(i, s, which).start()

        zero_q = jnp.zeros((16, HEAD), BF16)
        for row in range(30):
            q32[pl.ds(row + row // 15, BBLK, stride=32), :] = q_ref[row, pl.ds(pl.multiple_of(i * BBLK, BBLK), BBLK), :].astype(F32)
        for bl in range(BBLK):
            ln = len_ref[i * BBLK + bl]
            q_b = q32[bl * 32:(bl + 1) * 32, :].astype(BF16)
            lhs = jnp.concatenate([jnp.concatenate([q_b[:16], zero_q], axis=1),
                                   jnp.concatenate([zero_q, q_b[16:]], axis=1)], axis=0)
            k_cat = jnp.concatenate([kbuf[s, bl, 0], kbuf[s, bl, 1]], axis=1)
            sc = lax.dot_general(lhs, k_cat, (((1,), (1,)), ((), ())), preferred_element_type=F32) * scale
            sc_v[bl * 32:(bl + 1) * 32, :] = jnp.where(gap <= ln, sc, -jnp.inf)
        for c in range(BBLK // 2):
            rows = slice(c * 64, (c + 1) * 64)
            sc = sc_v[rows, :]
            ex = jnp.exp(sc - jnp.max(sc, axis=1, keepdims=True))
            ex_v[rows, :] = ex.astype(BF16)
            den_v[rows, :] = jnp.broadcast_to(jnp.sum(ex, axis=1, keepdims=True), (64, HEAD))
        for bl in range(BBLK):
            v_cat = jnp.concatenate([vbuf[s, bl, 0], vbuf[s, bl, 1]], axis=1)
            mix = jnp.dot(ex_v[bl * 32:(bl + 1) * 32, :], v_cat, preferred_element_type=F32)
            o32[bl * 32:bl * 32 + 16, :] = mix[:16, :HEAD] / den_v[bl * 32:bl * 32 + 16, :]
            o32[bl * 32 + 16:bl * 32 + 32, :] = mix[16:, HEAD:] / den_v[bl * 32 + 16:bl * 32 + 32, :]
        for t in range(STEPS):
            for hd in range(Q_LOC):
                row = (hd // GROUP) * 16 + t * GROUP + hd % GROUP
                slab = o32[pl.ds(row, BBLK, stride=32), :]
                o_buf[i % 2, t, :, hd * HEAD:(hd + 1) * HEAD] = slab.astype(BF16)
        for t in range(STEPS):
            o_copy(i, t).start()

    loop(N_BLK, block)
    for i in range(N_BLK - 2, N_BLK):
        for which in PAIR:
            out_copy(i, i % SLOTS, which).wait()
        for t in range(STEPS):
            o_copy(i, t).wait()


def run_attn(lengths, q32, k_new, v_new, k_cache, v_cache):
    return pl.pallas_call(
        attn_kernel,
        out_shape=(jax.ShapeDtypeStruct((STEPS, BATCH, Q_W), BF16),
                   jax.ShapeDtypeStruct(k_cache.shape, BF16),
                   jax.ShapeDtypeStruct(v_cache.shape, BF16)),
        in_specs=[SM, HB, HB, HB, HB, HB],
        out_specs=(HB, HB, HB),
        scratch_shapes=[
            pltpu.VMEM((SLOTS, BBLK, KV_LOC, SEQ, HEAD), BF16),
            pltpu.VMEM((SLOTS, BBLK, KV_LOC, SEQ, HEAD), BF16),
            pltpu.VMEM((BBLK * 32, HEAD), F32),
            pltpu.VMEM((BBLK * 32, HEAD), F32),
            pltpu.VMEM((BBLK * 32, SEQ), F32),
            pltpu.VMEM((BBLK * 32, SEQ), BF16),
            pltpu.VMEM((BBLK * 32, HEAD), F32),
            pltpu.VMEM((2, STEPS, BBLK, Q_W), BF16),
            pltpu.VMEM((30, BATCH, HEAD), BF16),
            pltpu.VMEM((ROWS, KV_W), BF16),
            pltpu.VMEM((ROWS, KV_W), BF16),
            pltpu.SemaphoreType.DMA((2, SLOTS)),
            pltpu.SemaphoreType.DMA((2, SLOTS)),
            pltpu.SemaphoreType.DMA((2, STEPS)),
            pltpu.SemaphoreType.DMA((3,)),
        ],
        compiler_params=pltpu.CompilerParams(vmem_limit_bytes=VMEM_ALL),
        name='attend',
    )(lengths, q32, k_new, v_new, k_cache, v_cache)


CHUNKS = (64, 64)
CROWS = tuple(STEPS * n for n in CHUNKS)
PIECES = 5
PW = 512
D_TILES = PIECES + PIECES
HALF_T = PIECES
RING = 3
RESID = 6
GW = PW // 2
G_TILES = pl.cdiv(FF_LOC, GW)
G_STREAM = G_TILES - RESID
G_EXTRA = G_STREAM - RESID
PHASES = (('g', G_STREAM), ('d', D_TILES), ('g', G_STREAM), ('d', D_TILES))
WO_PER = D_MODEL // Q_W
WO_SLOTS = pl.cdiv(D_TILES, WO_PER)
WO_AHEAD = 2
B_LAG = 2
NORM_ROWS = 32
WHOLE = 2
TAIL_ROWS = ((0, 2 * CHUNKS[1]), (2 * CHUNKS[1], CHUNKS[1]))


def mlp_kernel(o_hbm, x_hbm, wo_hbm, w1_hbm, w3_hbm, w2_hbm, ga_hbm, gm_hbm,
               y_hbm,
               xh0, xh1, u0, ssq, ps0, ps1, pr0, pr1, r10, r11, r20, r21, a0, a1, ring, ga_ref, gm_ref, gain_f,
               in_sem, g_sem, wo_sem, ring_sem, res_sem, out_sem,
               p_send, p_recv, c_send, c_recv, a_send, a_recv, t_send, t_recv):
    me = lax.axis_index('tp')
    core = me % 2
    chip = me // 2
    mate = chip * 2 + (1 - core)
    peer = (1 - chip) * 2 + core
    xh = (xh0, xh1)
    u_v = [u0.at[pl.ds(0, n), :] for n in CROWS]
    p_out, p_in = (ps0, ps1), (pr0, pr1)
    r_v = ((r10, r11), (r20, r21))
    a_v = (a0, a1)
    firsts = (0, CHUNKS[0])

    barrier = pltpu.get_barrier_semaphore()
    for dev in (mate, peer):
        pl.semaphore_signal(barrier, inc=1, device_id={'tp': dev}, device_id_type=MESH)

    bases = []
    total = 0
    for _, n in PHASES:
        bases.append(total)
        total += n

    def out_col(i):
        k = i // 2
        own = i % 2
        half = own * core + (1 - own) * (1 - core)
        return half * HALF_T + k

    def g_col(i):
        return pl.multiple_of(jnp.minimum(i * GW, FF_LOC - GW), 128)

    def g_tile(s):
        return jnp.where(s < G_EXTRA, G_TILES - G_EXTRA + s, 2 * (s - G_EXTRA))

    def tile_copies(kind, idx, slot, sem):
        if kind == 'd':
            col = pl.multiple_of(out_col(idx) * PW, PW)
            return [pltpu.make_async_copy(w2_hbm.at[:, pl.ds(col, PW)], ring.at[slot, pl.ds(0, FF_LOC), :], sem.at[0])]
        col = g_col(idx)
        return [pltpu.make_async_copy(w1_hbm.at[:, pl.ds(col, GW)], ring.at[slot, :, pl.ds(0, GW)], sem.at[0]),
                pltpu.make_async_copy(w3_hbm.at[:, pl.ds(col, GW)], ring.at[slot, :, pl.ds(GW, GW)], sem.at[1])]

    def stream(ph, s, start):
        kind = PHASES[ph][0]
        slot = (bases[ph] + s) % RING
        idx = g_tile(s) if kind == 'g' else s
        for cp in tile_copies(kind, idx, slot, ring_sem.at[slot]):
            if start:
                cp.start()
            else:
                cp.wait()
        return slot

    def refill(ph, s):
        n = PHASES[ph][1]

        @pl.when(s + RING < n)
        def _():
            stream(ph, s + RING, True)

        if ph + 1 < len(PHASES):
            @pl.when(s + RING >= n)
            def _():
                stream(ph + 1, s + RING - n, True)

    o_copies, x_copies = [], []
    for ch in PAIR:
        for t in range(STEPS):
            o_copies.append(pltpu.make_async_copy(
                o_hbm.at[t, pl.ds(firsts[ch], CHUNKS[ch]), :],
                xh[ch].at[pl.ds(t * CHUNKS[ch], CHUNKS[ch]), pl.ds(0, Q_W)], in_sem.at[0, ch, t]))
            x_copies.append(pltpu.make_async_copy(
                x_hbm.at[t, pl.ds(firsts[ch], CHUNKS[ch]), :],
                xh[ch].at[pl.ds(t * CHUNKS[ch], CHUNKS[ch]), :], in_sem.at[1, ch, t]))
    g_copies = [pltpu.make_async_copy(ga_hbm, ga_ref, g_sem.at[0]), pltpu.make_async_copy(gm_hbm, gm_ref, g_sem.at[1])]
    for cp in o_copies + g_copies:
        cp.start()
    def wo_copy(i):
        col = pl.multiple_of(out_col(i) * PW, PW)
        rows = pl.ds(pl.multiple_of((i % WO_PER) * Q_W, Q_W), Q_W)
        return pltpu.make_async_copy(wo_hbm.at[:, pl.ds(col, PW)], ring.at[RING + i // WO_PER, rows, :], wo_sem.at[i])

    def res_copies(r):
        return tile_copies('g', 2 * r + 1, RING + r, res_sem.at[r])

    for i in range(WO_AHEAD):
        wo_copy(i).start()

    def mate_copy(ex, ch, k):
        return pltpu.make_async_remote_copy(
            src_ref=p_out[ch].at[k], dst_ref=p_in[ch].at[k], send_sem=p_send.at[ex, ch, k], recv_sem=p_recv.at[ex, ch, k],
            device_id={'tp': mate}, device_id_type=MESH)

    def peer_copy(ex, ch, k):
        return pltpu.make_async_remote_copy(
            src_ref=a_v[ch].at[core * HALF_T + k], dst_ref=r_v[ex][ch].at[k], send_sem=c_send.at[ex, ch, k], recv_sem=c_recv.at[ex, ch, k],
            device_id={'tp': peer}, device_id_type=MESH)

    def gather_copy(ex, ch, k, half):
        j = half * HALF_T + k
        return pltpu.make_async_remote_copy(
            src_ref=a_v[ch].at[j], dst_ref=a_v[ch].at[j], send_sem=a_send.at[ex, ch, k], recv_sem=a_recv.at[ex, ch, k],
            device_id={'tp': mate}, device_id_type=MESH)

    def tail_peer(g, k):
        rows = pl.ds(*TAIL_ROWS[g])
        return pltpu.make_async_remote_copy(
            src_ref=a_v[1].at[core * HALF_T + k, rows], dst_ref=r_v[1][1].at[k, rows],
            send_sem=t_send.at[0, g, k - WHOLE], recv_sem=t_recv.at[0, g, k - WHOLE],
            device_id={'tp': peer}, device_id_type=MESH)

    def tail_gather(g, k, half):
        rows = pl.ds(*TAIL_ROWS[g])
        j = half * HALF_T + k
        return pltpu.make_async_remote_copy(
            src_ref=a_v[1].at[j, rows], dst_ref=a_v[1].at[j, rows],
            send_sem=t_send.at[1, g, k - WHOLE], recv_sem=t_recv.at[1, g, k - WHOLE],
            device_id={'tp': mate}, device_id_type=MESH)

    def pair_sum(ex, ch, k):
        mate_copy(ex, ch, k).wait_recv()
        own = core * HALF_T + k
        a_v[ch][own] = (a_v[ch][own].astype(F32) + p_in[ch][k].astype(F32)).astype(BF16)

    def full_sum(ex, ch, k):
        peer_copy(ex, ch, k).wait()
        own = core * HALF_T + k
        a_v[ch][own] = (a_v[ch][own].astype(F32) + r_v[ex][ch][k].astype(F32)).astype(BF16)
        gather_copy(ex, ch, k, core).start()

    def sends_done(ex, ch):
        def step(k, _):
            gather_copy(ex, ch, k, core).wait_send()
            mate_copy(ex, ch, k).wait_send()
        loop(PIECES, step)

    def gather_done(ex, ch):
        def step(k, _):
            gather_copy(ex, ch, k, 1 - core).wait_recv()
        loop(PIECES, step)
        sends_done(ex, ch)

    def full_sums(ex, ch):
        def step(k, _):
            full_sum(ex, ch, k)
        loop(PIECES, step)

    def norm_add(ch, which, then=None, steps=range(STEPS), squares=None):
        def step(b, _):
            rows = pl.ds(pl.multiple_of(b * NORM_ROWS, NORM_ROWS), NORM_ROWS)
            if squares is None:
                acc = jnp.zeros((NORM_ROWS, PW), F32)
                for j in range(D_TILES):
                    val = a_v[ch][j, rows, :].astype(F32)
                    acc = acc + val * val
            else:
                acc = squares[rows, :]
            fac = lax.rsqrt(jnp.sum(acc, axis=1, keepdims=True) / float(D_MODEL) + NORM_EPS)
            for j in range(D_MODEL // HEAD):
                cols = slice(j * HEAD, (j + 1) * HEAD)
                val = a_v[ch][j * HEAD // PW, rows, j * HEAD % PW:j * HEAD % PW + HEAD].astype(F32)
                base = xh[ch][rows, cols].astype(F32)
                xh[ch][rows, cols] = (base + val * fac * jnp.concatenate([gain_f[which, :, cols]] * (NORM_ROWS // 8))).astype(BF16)
        for t in steps:
            loop((t + 1) * CHUNKS[ch] // NORM_ROWS, step, t * CHUNKS[ch] // NORM_ROWS)
            if then is not None:
                then(t)

    for cp in o_copies + g_copies:
        cp.wait()

    def wo_tile(i, ch):
        rows = pl.ds(pl.multiple_of((i % WO_PER) * Q_W, Q_W), Q_W)
        return jnp.dot(xh[ch][:, pl.ds(0, Q_W)], ring[RING + i // WO_PER, rows, :],
                       preferred_element_type=F32).astype(BF16)

    def wo_sweep(ch):
        def step(k, _):
            if ch == 0:
                wo_copy(2 * k).wait()
                wo_copy(2 * k + 1).wait()

                @pl.when(2 * k + WO_AHEAD < D_TILES)
                def _():
                    wo_copy(2 * k + WO_AHEAD).start()
                    wo_copy(2 * k + WO_AHEAD + 1).start()
            p_out[ch][k] = wo_tile(2 * k, ch)
            mate_copy(0, ch, k).start()
            a_v[ch][core * HALF_T + k] = wo_tile(2 * k + 1, ch)

            pair_sum(0, ch, k)
            if ch == 0:
                peer_copy(0, ch, k).start()
        loop(PIECES, step)

    pl.semaphore_wait(barrier, 2)
    with jax.named_scope('wo'):
        wo_sweep(0)
        for n in range(RING):
            stream(0, n, True)
        for r in range(WO_SLOTS, RESID):
            for cp in res_copies(r):
                cp.start()
        wo_sweep(1)

    for cp in x_copies:
        cp.start()
    for r in range(WO_SLOTS):
        for cp in res_copies(r):
            cp.start()
    with jax.named_scope('sums_a1'):
        def add_squares(val):
            for c in range(0, PW, HEAD):
                part = val[:, c:c + HEAD]
                ssq[...] = ssq[...] + part * part

        def mate_square(k):
            gather_copy(0, 0, k, 1 - core).wait_recv()
            val = a_v[0][(1 - core) * HALF_T + k].astype(F32)
            add_squares(val)

        ssq[...] = jnp.zeros_like(ssq)
        for which, gain_ref in enumerate((ga_ref, gm_ref)):
            for j in range(D_MODEL // HEAD):
                row = gain_ref[j:j + 1, :].astype(F32)
                gain_f[which, :, j * HEAD:(j + 1) * HEAD] = jnp.broadcast_to(row, (8, HEAD))

        def first_sums(k, _):
            full_sum(0, 0, k)
            val = a_v[0][core * HALF_T + k].astype(F32)
            add_squares(val)

            @pl.when(k >= 1)
            def _():
                mate_square(k - 1)

            @pl.when(k >= B_LAG)
            def _():
                peer_copy(0, 1, k - B_LAG).start()
        loop(PIECES, first_sums)
        for k in range(PIECES - B_LAG, PIECES):
            peer_copy(0, 1, k).start()
    with jax.named_scope('gather_a1'):
        mate_square(PIECES - 1)
    for cp in x_copies:
        cp.wait()
    with jax.named_scope('norm_a1'):
        norm_add(0, 0, squares=ssq)
        sends_done(0, 0)

    def gate_up(ph, ch):
        def tile(i, slot):
            acc = jnp.dot(xh[ch][...], ring[slot], preferred_element_type=F32)
            gate = acc[:, :GW]
            act = (gate * jax.nn.sigmoid(gate)) * acc[:, GW:]
            u_v[ch][:, pl.ds(g_col(i), GW)] = act.astype(BF16)

        def single(q, _):
            tile(g_tile(q), stream(ph, q, False))
            refill(ph, q)

        def pair(q, _):
            slot = stream(ph, G_EXTRA + q, False)
            if ph == 0:
                for cp in res_copies(q):
                    cp.wait()
            tile(2 * q, slot)
            tile(2 * q + 1, RING + q)
            refill(ph, G_EXTRA + q)
        loop(G_EXTRA, single)
        loop(RESID, pair)

    def down(ph, ch, also, lag):
        def swap(k):
            pair_sum(1, ch, k)
            peer_copy(1, ch, k).start()

        def d_tile(i):
            slot = stream(ph, i, False)
            res = jnp.dot(u_v[ch][...], ring[slot, pl.ds(0, FF_LOC), :], preferred_element_type=F32).astype(BF16)
            refill(ph, i)
            return res

        def step(k, _):
            also(k)
            p_out[ch][k] = d_tile(2 * k)
            mate_copy(1, ch, k).start()

            if lag:
                @pl.when(k >= 1)
                def _():
                    swap(k - 1)
            a_v[ch][core * HALF_T + k] = d_tile(2 * k + 1)
            if not lag:
                pair_sum(1, ch, k)

                @pl.when(k < WHOLE)
                def _():
                    peer_copy(1, ch, k).start()
        loop(PIECES, step)


    with jax.named_scope('gate_up_a'):
        gate_up(0, 0)
    with jax.named_scope('down_a'):
        down(1, 0, lambda k: full_sum(0, 1, k), True)
    with jax.named_scope('gather_b1'):
        gather_done(0, 1)
    with jax.named_scope('norm_b1'):
        norm_add(1, 0)
        pair_sum(1, 0, PIECES - 1)
        peer_copy(1, 0, PIECES - 1).start()
    with jax.named_scope('gate_up_b'):
        gate_up(2, 1)
    with jax.named_scope('down_b'):
        down(3, 1, lambda k: full_sum(1, 0, k), False)
        for g in PAIR:
            for k in range(WHOLE, PIECES):
                tail_peer(g, k).start()

    def y_copies(ch):
        return [pltpu.make_async_copy(xh[ch].at[pl.ds(t * CHUNKS[ch], CHUNKS[ch]), :],
                                      y_hbm.at[t, pl.ds(firsts[ch], CHUNKS[ch]), :], out_sem.at[ch, t]) for t in range(STEPS)]

    with jax.named_scope('gather_a2'):
        gather_done(1, 0)
    with jax.named_scope('norm_a2'):
        norm_add(0, 1, lambda t: y_copies(0)[t].start())
    with jax.named_scope('sums_b2'):
        def whole_sums(k, _):
            full_sum(1, 1, k)
        loop(WHOLE, whole_sums)
    for g in PAIR:
        rows = pl.ds(*TAIL_ROWS[g])
        with jax.named_scope(f'sums_b2#g={g}'):
            for k in range(WHOLE, PIECES):
                own = core * HALF_T + k
                tail_peer(g, k).wait()
                a_v[1][own, rows, :] = (a_v[1][own, rows, :].astype(F32) + r_v[1][1][k, rows, :].astype(F32)).astype(BF16)
                tail_gather(g, k, core).start()
        with jax.named_scope(f'gather_b2#g={g}'):
            if g == 0:
                def whole_done(k, _):
                    gather_copy(1, 1, k, core).wait_send()
                    gather_copy(1, 1, k, 1 - core).wait_recv()
                loop(WHOLE, whole_done)

                def mates_done(k, _):
                    mate_copy(1, 1, k).wait_send()
                loop(PIECES, mates_done)
            for k in range(WHOLE, PIECES):
                tail_gather(g, k, core).wait_send()
                tail_gather(g, k, 1 - core).wait_recv()
        with jax.named_scope(f'norm_b2#g={g}'):
            norm_add(1, 1, lambda t: y_copies(1)[t].start(), ((0, 1), (2,))[g])
    with jax.named_scope('y_out'):
        for ch in PAIR:
            for cp in y_copies(ch):
                cp.wait()


def run_mlp(o, x_seq, w_o, w_gate, w_up, w_down, g_a, g_m):
    sem = pltpu.SemaphoreType.DMA
    return pl.pallas_call(
        mlp_kernel,
        out_shape=jax.ShapeDtypeStruct((STEPS, BATCH, D_MODEL), BF16),
        in_specs=[HB] * 8,
        out_specs=HB,
        scratch_shapes=[
            *[pltpu.VMEM((n, D_MODEL), BF16) for n in CROWS],
            pltpu.VMEM((max(CROWS), FF_LOC), BF16),
            pltpu.VMEM((CROWS[0], HEAD), F32),
            *[pltpu.VMEM((PIECES, n, PW), BF16) for n in CROWS * 4],
            *[pltpu.VMEM((D_TILES, n, PW), BF16) for n in CROWS],
            pltpu.VMEM((RING + RESID, D_MODEL, PW), BF16),
            *[pltpu.VMEM((D_MODEL // HEAD, HEAD), BF16)] * 2,
            pltpu.VMEM((2, 8, D_MODEL), F32),
            sem((2, 2, STEPS)), sem((2,)), sem((D_TILES,)), sem((RING, 2)), sem((RESID, 2)), sem((2, STEPS)),
            *[sem((2, 2, PIECES))] * 6,
            *[sem((2, 2, PIECES - WHOLE))] * 2,
        ],
        compiler_params=pltpu.CompilerParams(collective_id=1, has_side_effects=True, vmem_limit_bytes=VMEM_ALL),
        name='wo_mlp',
    )(o, x_seq, w_o, w_gate, w_up, w_down, g_a, g_m)


def solution(mesh):
    def local_run(x_seq, cache_len, k_cache, v_cache, w_q, w_k, w_v, w_o, w_gate, w_up, w_down, g_q, g_k, g_attn, g_mlp):
        inv_freq = ROPE_THETA ** (-(np.arange(HEAD // 2, dtype=np.float32) * np.float32(2.0 / HEAD)))
        freq_row = jnp.asarray(np.concatenate([inv_freq, inv_freq])[None, :], dtype=F32)
        tiled = lambda g: g.reshape(-1, HEAD)
        q_rot, k_new, v_new = run_qkv(x_seq.reshape(ROWS, D_MODEL), w_q, w_k, w_v, tiled(g_q), tiled(g_k), cache_len[None, :], freq_row)
        o, k_out, v_out = run_attn(cache_len, q_rot, k_new, v_new, k_cache, v_cache)
        y = run_mlp(o, x_seq, w_o, w_gate, w_up, w_down, tiled(g_attn), tiled(g_mlp))
        return y, k_out, v_out

    data_spec = P(None, 'dp')
    cache_spec = P('dp', 'tp')
    col_spec = P(None, 'tp')
    row_spec = P('tp')
    arg_specs = (data_spec, P('dp'), cache_spec, cache_spec, col_spec, col_spec, col_spec, row_spec, col_spec, col_spec, row_spec, P('tp'), P('tp'), P(), P())
    out_specs = (data_spec, cache_spec, cache_spec)
    return jax.shard_map(local_run, mesh=mesh, in_specs=arg_specs, out_specs=out_specs, check_vma=False)
```

```python
import jax
import jax.numpy as jnp
import numpy as np
from jax import lax
from jax.experimental import pallas as pl
from jax.experimental.pallas import tpu as pltpu
from jax.sharding import PartitionSpec as P

ROPE_THETA = 500000.0
NORM_EPS = 1e-6
MESH = pl.DeviceIdType.MESH
F32 = jnp.float32
PAIR = range(2)
VMEM_ALL = 67043328
BF16 = jnp.bfloat16

STEPS = 3
BATCH = 128
ROWS = STEPS * BATCH
D_MODEL = 5120
HEAD = 128
KV_LOC = 2
GROUP = 5
Q_LOC = KV_LOC * GROUP
SEQ = 256
FF_LOC = 3456
KV_W = KV_LOC * HEAD
Q_W = Q_LOC * HEAD

ANY = pl.BlockSpec(memory_space=pl.ANY)
VM = pl.BlockSpec(memory_space=pltpu.VMEM)
SM = pl.BlockSpec(memory_space=pltpu.SMEM)
HB = pl.BlockSpec(memory_space=pltpu.HBM)


def loop(stop, body, start=0):
    def step(i, carry):
        body(i, carry)
        return carry
    lax.fori_loop(start, stop, step, 0)


N_TILE = 512


def qkv_kernel(x_hbm, wq_hbm, wk_hbm, wv_hbm, gq_hbm, gk_hbm, len_hbm, freq_hbm,
               q_hbm, k_hbm, v_hbm,
               x_v, w_v, raw, cos_v, sin_v, sq_acc, sq_own, sq_recv, q_v, k_v, v_v, gq_v, gk_v, len_v, freq_v,
               x_sem, w_sem, send_sem, recv_sem, t_sem, o_sem):
    me = lax.axis_index('tp')
    barrier = pltpu.get_barrier_semaphore()
    for d in range(1, 4):
        pl.semaphore_signal(barrier, inc=1, device_id={'tp': (me + d) % 4}, device_id_type=MESH)

    half_k = D_MODEL // 2
    halves = [pl.ds(n * half_k, half_k) for n in PAIR]
    x_copies = [pltpu.make_async_copy(x_hbm.at[:, h], x_v.at[:, h], x_sem.at[n]) for n, h in enumerate(halves)]
    w_copies = [
        [pltpu.make_async_copy(wq_hbm.at[h, pl.ds(0, N_TILE)], w_v.at[0, h], w_sem.at[n]) for n, h in enumerate(halves)],
        [pltpu.make_async_copy(wq_hbm.at[:, pl.ds(N_TILE, N_TILE)], w_v.at[1], w_sem.at[2])],
        [pltpu.make_async_copy(wq_hbm.at[:, pl.ds(1024, 256)], w_v.at[2, :, pl.ds(0, 256)], w_sem.at[3]),
         pltpu.make_async_copy(wk_hbm, w_v.at[2, :, pl.ds(256, 256)], w_sem.at[4])],
        [pltpu.make_async_copy(wv_hbm, w_v.at[3, :, pl.ds(0, 256)], w_sem.at[5])],
    ]
    t_copies = [pltpu.make_async_copy(src, dst, t_sem.at[n])
                for n, (src, dst) in enumerate(((len_hbm, len_v), (freq_hbm, freq_v), (gq_hbm, gq_v), (gk_hbm, gk_v)))]
    for cp in t_copies:
        cp.start()
    x_copies[0].start()
    w_copies[0][0].start()

    for cp in t_copies:
        cp.wait()
    len_col = jnp.transpose(jnp.broadcast_to(len_v[...].astype(F32), (HEAD, BATCH)))
    sign = jnp.where(lax.broadcasted_iota(jnp.int32, (BATCH, HEAD), 1) < HEAD // 2, -1.0, 1.0)
    for t in range(STEPS):
        rows = pl.ds(t * BATCH, BATCH)
        ang = (len_col + float(t)) * freq_v[...]
        cos_v[rows, :] = jnp.cos(ang)
        sin_v[rows, :] = jnp.sin(ang) * sign

    x_copies[1].start()
    w_copies[0][1].start()

    def piece(col, rows):
        return raw[col // N_TILE, rows, col % N_TILE:col % N_TILE + HEAD]

    def square(cols, rows, acc):
        for col in cols:
            val = piece(col, rows)
            acc = acc + val * val
        return acc

    all_rows = [pl.ds(t * BATCH, BATCH) for t in range(STEPS)]
    zero = jnp.zeros((BATCH, HEAD), F32)

    half_rows = [pl.ds(n * (ROWS // 2), ROWS // 2) for n in PAIR]

    def tile_dot(i, ks=slice(None)):
        return [jnp.dot(x_v[rows, ks], w_v[i, ks, :], preferred_element_type=F32) for rows in half_rows]

    def keep(i, parts):
        for rows, part in zip(half_rows, parts):
            raw[i, rows, :] = part.astype(BF16).astype(F32)

    x_copies[0].wait()
    w_copies[0][0].wait()
    w_copies[1][0].start()
    for rows, part in zip(half_rows, tile_dot(0, halves[0])):
        raw[0, rows, :] = part
    x_copies[1].wait()
    w_copies[0][1].wait()
    for cp in w_copies[2]:
        cp.start()
    keep(0, [raw[0, rows, :] + part for rows, part in zip(half_rows, tile_dot(0, halves[1]))])
    w_copies[1][0].wait()
    w_copies[3][0].start()
    keep(1, tile_dot(1))
    for cp in w_copies[2]:
        cp.wait()
    for t in range(STEPS):
        sq_acc[all_rows[t], :] = square(range(0, 1024, HEAD), all_rows[t], zero)
    keep(2, tile_dot(2))
    w_copies[3][0].wait()

    first_row = lax.broadcasted_iota(jnp.int32, (8, BATCH), 0) == 0
    for t in range(STEPS):
        rows = all_rows[t]
        sums = [jnp.sum(jnp.transpose(acc), axis=0, keepdims=True)
                for acc in (square(range(1024, 1280, HEAD), rows, sq_acc[rows, :]), square(range(1280, 1536, HEAD), rows, zero))]
        sq_own[:, t * BATCH:(t + 1) * BATCH] = jnp.where(first_row, sums[0], sums[1])

    with jax.named_scope('k1_barrier'):
        pl.semaphore_wait(barrier, 3)
    copies = []
    for d in range(1, 4):
        cp = pltpu.make_async_remote_copy(
            src_ref=sq_own, dst_ref=sq_recv.at[d - 1], send_sem=send_sem.at[d - 1], recv_sem=recv_sem.at[d - 1],
            device_id={'tp': (me + d) % 4}, device_id_type=MESH)
        cp.start()
        copies.append(cp)
    for rows in half_rows:
        v_v[rows, :] = jnp.dot(x_v[rows, :], w_v[3, :, pl.ds(0, 256)], preferred_element_type=F32).astype(BF16)
    outs = [pltpu.make_async_copy(v_v, v_hbm, o_sem.at[0])]
    outs[0].start()
    with jax.named_scope('k1_recv'):
        for cp in copies:
            cp.wait()

    q_width = float(Q_LOC * HEAD * 4)
    k_width = float(KV_LOC * HEAD * 4)
    for t in range(STEPS):
        cols = slice(t * BATCH, (t + 1) * BATCH)
        rows = all_rows[t]
        tot = sq_own[:, cols] + sq_recv[0, :, cols] + sq_recv[1, :, cols] + sq_recv[2, :, cols]
        q_fac = lax.rsqrt(tot[0:1] / q_width + NORM_EPS)
        k_fac = lax.rsqrt(tot[1:2] / k_width + NORM_EPS)
        q_col = jnp.transpose(jnp.broadcast_to(q_fac, (HEAD, BATCH)))
        k_col = jnp.transpose(jnp.broadcast_to(k_fac, (HEAD, BATCH)))
        cos_t = cos_v[rows, :]
        sin_t = sin_v[rows, :]
        for hd in range(Q_LOC):
            val = piece(hd * HEAD, rows) * q_col * gq_v[hd:hd + 1, :].astype(F32)
            rot = val * cos_t + pltpu.roll(val, HEAD // 2, 1) * sin_t
            q_v[(hd // GROUP) * 15 + t * GROUP + hd % GROUP] = rot.astype(BF16)
        for kv in range(KV_LOC):
            val = piece((Q_LOC + kv) * HEAD, rows) * k_col * gk_v[kv:kv + 1, :].astype(F32)
            rot = val * cos_t + pltpu.roll(val, HEAD // 2, 1) * sin_t
            k_v[rows, kv * HEAD:(kv + 1) * HEAD] = rot.astype(BF16)
        for kv in range(KV_LOC):
            slabs = pl.ds(kv * 15 + t * GROUP, GROUP)
            outs.append(pltpu.make_async_copy(q_v.at[slabs], q_hbm.at[slabs], o_sem.at[len(outs)]))
        outs.append(pltpu.make_async_copy(k_v.at[rows], k_hbm.at[rows], o_sem.at[len(outs)]))
        for cp in outs[-3:]:
            cp.start()
    with jax.named_scope('k1_out'):
        for cp in outs:
            cp.wait()


def run_qkv(x2, w_q, w_k, w_v, g_q, g_k, len_row, freq_row):
    return pl.pallas_call(
        qkv_kernel,
        out_shape=(jax.ShapeDtypeStruct((30, BATCH, HEAD), BF16),
                   jax.ShapeDtypeStruct((ROWS, KV_W), BF16),
                   jax.ShapeDtypeStruct((ROWS, KV_W), BF16)),
        in_specs=[HB] * 8,
        out_specs=(HB, HB, HB),
        scratch_shapes=[
            pltpu.VMEM((ROWS, D_MODEL), BF16),
            pltpu.VMEM((4, D_MODEL, N_TILE), BF16),
            pltpu.VMEM((3, ROWS, N_TILE), F32),
            *[pltpu.VMEM((ROWS, HEAD), F32)] * 3,
            pltpu.VMEM((8, ROWS), F32),
            pltpu.VMEM((3, 8, ROWS), F32),
            pltpu.VMEM((30, BATCH, HEAD), BF16),
            pltpu.VMEM((ROWS, KV_W), BF16),
            pltpu.VMEM((ROWS, KV_W), BF16),
            pltpu.VMEM((Q_LOC, HEAD), BF16),
            pltpu.VMEM((KV_LOC, HEAD), BF16),
            pltpu.VMEM((1, BATCH), jnp.int32),
            pltpu.VMEM((1, HEAD), F32),
            *[pltpu.SemaphoreType.DMA((n,)) for n in (2, 6, 3, 3, 4, 10)],
        ],
        compiler_params=pltpu.CompilerParams(collective_id=0, has_side_effects=True, vmem_limit_bytes=VMEM_ALL),
        name='qkv_rope',
    )(x2, w_q, w_k, w_v, g_q, g_k, len_row, freq_row)


BBLK = 16
N_BLK = BATCH // BBLK
SLOTS = 4


def attn_kernel(len_ref, q_hbm, kn_hbm, vn_hbm, kc_hbm, vc_hbm,
                o_hbm, ko_hbm, vo_hbm,
                kbuf, vbuf, q32, o32, sc_v, ex_v, den_v, o_buf, q_ref, kn_ref, vn_ref, in_sem, out_sem, o_sem, t_sem):
    def in_copy(i, s, which):
        src = (kc_hbm, vc_hbm)[which]
        dst = (kbuf, vbuf)[which]
        return pltpu.make_async_copy(src.at[pl.ds(i * BBLK, BBLK)], dst.at[s], in_sem.at[which, s])

    def out_copy(i, s, which):
        dst = (ko_hbm, vo_hbm)[which]
        src = (kbuf, vbuf)[which]
        return pltpu.make_async_copy(src.at[s], dst.at[pl.ds(i * BBLK, BBLK)], out_sem.at[which, s])

    def o_copy(i, t):
        return pltpu.make_async_copy(o_buf.at[i % 2, t], o_hbm.at[t, pl.ds(pl.multiple_of(i * BBLK, BBLK), BBLK), :], o_sem.at[i % 2, t])

    t_copies = [pltpu.make_async_copy(src, dst, t_sem.at[n])
                for n, (src, dst) in enumerate(((kn_hbm, kn_ref), (vn_hbm, vn_ref), (q_hbm, q_ref)))]
    for cp in t_copies:
        cp.start()
    for i in PAIR:
        for which in PAIR:
            in_copy(i, i, which).start()
    for pad in (15, 31):
        q32[pl.ds(pad, BBLK, stride=32), :] = jnp.zeros((BBLK, HEAD), F32)

    scale = HEAD ** -0.5
    row_id = lax.broadcasted_iota(jnp.int32, (32, SEQ), 0)
    col_id = lax.broadcasted_iota(jnp.int32, (32, SEQ), 1)
    sub = row_id - jnp.where(row_id >= 16, 16, 0)
    step_of = jnp.where(sub >= 5, 1, 0) + jnp.where(sub >= 10, 1, 0)
    gap = col_id - step_of
    win_id = lax.broadcasted_iota(jnp.int32, (32, HEAD), 0)

    for cp in t_copies:
        cp.wait()

    def block(i, _):
        s = i % SLOTS

        @pl.when(i >= 2)
        def _():
            for which in PAIR:
                out_copy(i - 2, (i + 2) % SLOTS, which).wait()
            for t in range(STEPS):
                o_copy(i - 2, t).wait()

        @pl.when(i + 2 < N_BLK)
        def _():
            for which in PAIR:
                in_copy(i + 2, (i + 2) % SLOTS, which).start()

        for which in PAIR:
            in_copy(i, s, which).wait()

        news = []
        for src in (kn_ref, vn_ref):
            news.append([src[pl.ds(pl.multiple_of(t * BATCH + i * BBLK, BBLK), BBLK), :].astype(F32) for t in range(STEPS)])
        for bl in range(BBLK):
            ln = len_ref[i * BBLK + bl]
            w0 = jnp.minimum((ln // 16) * 16, SEQ - 32)
            win = pl.ds(pl.multiple_of(w0, 16), 32)
            rel = win_id - (ln - w0)
            for buf, new in ((kbuf, news[0]), (vbuf, news[1])):
                for kv in range(KV_LOC):
                    val = buf[s, bl, kv, win, :].astype(F32)
                    for t in range(STEPS):
                        row = new[t][bl:bl + 1, kv * HEAD:(kv + 1) * HEAD]
                        val = jnp.where(rel == t, jnp.broadcast_to(row, (32, HEAD)), val)
                    buf[s, bl, kv, win, :] = val.astype(BF16)
        for which in PAIR:
            out_copy(i, s, which).start()

        zero_q = jnp.zeros((16, HEAD), BF16)
        for row in range(30):
            q32[pl.ds(row + row // 15, BBLK, stride=32), :] = q_ref[row, pl.ds(pl.multiple_of(i * BBLK, BBLK), BBLK), :].astype(F32)
        for bl in range(BBLK):
            ln = len_ref[i * BBLK + bl]
            q_b = q32[bl * 32:(bl + 1) * 32, :].astype(BF16)
            lhs = jnp.concatenate([jnp.concatenate([q_b[:16], zero_q], axis=1),
                                   jnp.concatenate([zero_q, q_b[16:]], axis=1)], axis=0)
            k_cat = jnp.concatenate([kbuf[s, bl, 0], kbuf[s, bl, 1]], axis=1)
            sc = lax.dot_general(lhs, k_cat, (((1,), (1,)), ((), ())), preferred_element_type=F32) * scale
            sc_v[bl * 32:(bl + 1) * 32, :] = jnp.where(gap <= ln, sc, -jnp.inf)
        for c in range(BBLK // 2):
            rows = slice(c * 64, (c + 1) * 64)
            sc = sc_v[rows, :]
            ex = jnp.exp(sc - jnp.max(sc, axis=1, keepdims=True))
            ex_v[rows, :] = ex.astype(BF16)
            den_v[rows, :] = jnp.broadcast_to(jnp.sum(ex, axis=1, keepdims=True), (64, HEAD))
        for bl in range(BBLK):
            v_cat = jnp.concatenate([vbuf[s, bl, 0], vbuf[s, bl, 1]], axis=1)
            mix = jnp.dot(ex_v[bl * 32:(bl + 1) * 32, :], v_cat, preferred_element_type=F32)
            o32[bl * 32:bl * 32 + 16, :] = mix[:16, :HEAD] / den_v[bl * 32:bl * 32 + 16, :]
            o32[bl * 32 + 16:bl * 32 + 32, :] = mix[16:, HEAD:] / den_v[bl * 32 + 16:bl * 32 + 32, :]
        for t in range(STEPS):
            for hd in range(Q_LOC):
                row = (hd // GROUP) * 16 + t * GROUP + hd % GROUP
                slab = o32[pl.ds(row, BBLK, stride=32), :]
                o_buf[i % 2, t, :, hd * HEAD:(hd + 1) * HEAD] = slab.astype(BF16)
        for t in range(STEPS):
            o_copy(i, t).start()

    loop(N_BLK, block)
    for i in range(N_BLK - 2, N_BLK):
        for which in PAIR:
            out_copy(i, i % SLOTS, which).wait()
        for t in range(STEPS):
            o_copy(i, t).wait()


def run_attn(lengths, q32, k_new, v_new, k_cache, v_cache):
    return pl.pallas_call(
        attn_kernel,
        out_shape=(jax.ShapeDtypeStruct((STEPS, BATCH, Q_W), BF16),
                   jax.ShapeDtypeStruct(k_cache.shape, BF16),
                   jax.ShapeDtypeStruct(v_cache.shape, BF16)),
        in_specs=[SM, HB, HB, HB, HB, HB],
        out_specs=(HB, HB, HB),
        scratch_shapes=[
            pltpu.VMEM((SLOTS, BBLK, KV_LOC, SEQ, HEAD), BF16),
            pltpu.VMEM((SLOTS, BBLK, KV_LOC, SEQ, HEAD), BF16),
            pltpu.VMEM((BBLK * 32, HEAD), F32),
            pltpu.VMEM((BBLK * 32, HEAD), F32),
            pltpu.VMEM((BBLK * 32, SEQ), F32),
            pltpu.VMEM((BBLK * 32, SEQ), BF16),
            pltpu.VMEM((BBLK * 32, HEAD), F32),
            pltpu.VMEM((2, STEPS, BBLK, Q_W), BF16),
            pltpu.VMEM((30, BATCH, HEAD), BF16),
            pltpu.VMEM((ROWS, KV_W), BF16),
            pltpu.VMEM((ROWS, KV_W), BF16),
            pltpu.SemaphoreType.DMA((2, SLOTS)),
            pltpu.SemaphoreType.DMA((2, SLOTS)),
            pltpu.SemaphoreType.DMA((2, STEPS)),
            pltpu.SemaphoreType.DMA((3,)),
        ],
        compiler_params=pltpu.CompilerParams(vmem_limit_bytes=VMEM_ALL),
        name='attend',
    )(lengths, q32, k_new, v_new, k_cache, v_cache)


CHUNKS = (64, 64)
CROWS = tuple(STEPS * n for n in CHUNKS)
PIECES = 5
PW = 512
D_TILES = PIECES + PIECES
HALF_T = PIECES
RING = 3
RESID = 6
GW = PW // 2
G_TILES = pl.cdiv(FF_LOC, GW)
G_STREAM = G_TILES - RESID
G_EXTRA = G_STREAM - RESID
PHASES = (('g', G_STREAM), ('d', D_TILES), ('g', G_STREAM), ('d', D_TILES))
WO_PER = D_MODEL // Q_W
WO_SLOTS = pl.cdiv(D_TILES, WO_PER)
WO_AHEAD = 2
B_LAG = 2
NORM_ROWS = 32
WHOLE = 2
TAIL_ROWS = ((0, 2 * CHUNKS[1]), (2 * CHUNKS[1], CHUNKS[1]))


def mlp_kernel(o_hbm, x_hbm, wo_hbm, w1_hbm, w3_hbm, w2_hbm, ga_hbm, gm_hbm,
               y_hbm,
               xh0, xh1, u0, ssq, ps0, ps1, pr0, pr1, r10, r11, r20, r21, a0, a1, ring, ga_ref, gm_ref, gain_f,
               in_sem, g_sem, wo_sem, ring_sem, res_sem, out_sem,
               p_send, p_recv, c_send, c_recv, a_send, a_recv, t_send, t_recv):
    me = lax.axis_index('tp')
    core = me % 2
    chip = me // 2
    mate = chip * 2 + (1 - core)
    peer = (1 - chip) * 2 + core
    xh = (xh0, xh1)
    u_v = [u0.at[pl.ds(0, n), :] for n in CROWS]
    p_out, p_in = (ps0, ps1), (pr0, pr1)
    r_v = ((r10, r11), (r20, r21))
    a_v = (a0, a1)
    firsts = (0, CHUNKS[0])

    barrier = pltpu.get_barrier_semaphore()
    for dev in (mate, peer):
        pl.semaphore_signal(barrier, inc=1, device_id={'tp': dev}, device_id_type=MESH)

    bases = []
    total = 0
    for _, n in PHASES:
        bases.append(total)
        total += n

    def out_col(i):
        k = i // 2
        own = i % 2
        half = own * core + (1 - own) * (1 - core)
        return half * HALF_T + k

    def g_col(i):
        return pl.multiple_of(jnp.minimum(i * GW, FF_LOC - GW), 128)

    def g_tile(s):
        return jnp.where(s < G_EXTRA, G_TILES - G_EXTRA + s, 2 * (s - G_EXTRA))

    def tile_copies(kind, idx, slot, sem):
        if kind == 'd':
            col = pl.multiple_of(out_col(idx) * PW, PW)
            return [pltpu.make_async_copy(w2_hbm.at[:, pl.ds(col, PW)], ring.at[slot, pl.ds(0, FF_LOC), :], sem.at[0])]
        col = g_col(idx)
        return [pltpu.make_async_copy(w1_hbm.at[:, pl.ds(col, GW)], ring.at[slot, :, pl.ds(0, GW)], sem.at[0]),
                pltpu.make_async_copy(w3_hbm.at[:, pl.ds(col, GW)], ring.at[slot, :, pl.ds(GW, GW)], sem.at[1])]

    def stream(ph, s, start):
        kind = PHASES[ph][0]
        slot = (bases[ph] + s) % RING
        idx = g_tile(s) if kind == 'g' else s
        for cp in tile_copies(kind, idx, slot, ring_sem.at[slot]):
            if start:
                cp.start()
            else:
                cp.wait()
        return slot

    def refill(ph, s):
        n = PHASES[ph][1]

        @pl.when(s + RING < n)
        def _():
            stream(ph, s + RING, True)

        if ph + 1 < len(PHASES):
            @pl.when(s + RING >= n)
            def _():
                stream(ph + 1, s + RING - n, True)

    o_copies, x_copies = [], []
    for ch in PAIR:
        for t in range(STEPS):
            o_copies.append(pltpu.make_async_copy(
                o_hbm.at[t, pl.ds(firsts[ch], CHUNKS[ch]), :],
                xh[ch].at[pl.ds(t * CHUNKS[ch], CHUNKS[ch]), pl.ds(0, Q_W)], in_sem.at[0, ch, t]))
            x_copies.append(pltpu.make_async_copy(
                x_hbm.at[t, pl.ds(firsts[ch], CHUNKS[ch]), :],
                xh[ch].at[pl.ds(t * CHUNKS[ch], CHUNKS[ch]), :], in_sem.at[1, ch, t]))
    g_copies = [pltpu.make_async_copy(ga_hbm, ga_ref, g_sem.at[0]), pltpu.make_async_copy(gm_hbm, gm_ref, g_sem.at[1])]
    for cp in o_copies + g_copies:
        cp.start()
    def wo_copy(i):
        col = pl.multiple_of(out_col(i) * PW, PW)
        rows = pl.ds(pl.multiple_of((i % WO_PER) * Q_W, Q_W), Q_W)
        return pltpu.make_async_copy(wo_hbm.at[:, pl.ds(col, PW)], ring.at[RING + i // WO_PER, rows, :], wo_sem.at[i])

    def res_copies(r):
        return tile_copies('g', 2 * r + 1, RING + r, res_sem.at[r])

    for i in range(WO_AHEAD):
        wo_copy(i).start()

    def mate_copy(ex, ch, k):
        return pltpu.make_async_remote_copy(
            src_ref=p_out[ch].at[k], dst_ref=p_in[ch].at[k], send_sem=p_send.at[ex, ch, k], recv_sem=p_recv.at[ex, ch, k],
            device_id={'tp': mate}, device_id_type=MESH)

    def peer_copy(ex, ch, k):
        return pltpu.make_async_remote_copy(
            src_ref=a_v[ch].at[core * HALF_T + k], dst_ref=r_v[ex][ch].at[k], send_sem=c_send.at[ex, ch, k], recv_sem=c_recv.at[ex, ch, k],
            device_id={'tp': peer}, device_id_type=MESH)

    def gather_copy(ex, ch, k, half):
        j = half * HALF_T + k
        return pltpu.make_async_remote_copy(
            src_ref=a_v[ch].at[j], dst_ref=a_v[ch].at[j], send_sem=a_send.at[ex, ch, k], recv_sem=a_recv.at[ex, ch, k],
            device_id={'tp': mate}, device_id_type=MESH)

    def tail_peer(g, k):
        rows = pl.ds(*TAIL_ROWS[g])
        return pltpu.make_async_remote_copy(
            src_ref=a_v[1].at[core * HALF_T + k, rows], dst_ref=r_v[1][1].at[k, rows],
            send_sem=t_send.at[0, g, k - WHOLE], recv_sem=t_recv.at[0, g, k - WHOLE],
            device_id={'tp': peer}, device_id_type=MESH)

    def tail_gather(g, k, half):
        rows = pl.ds(*TAIL_ROWS[g])
        j = half * HALF_T + k
        return pltpu.make_async_remote_copy(
            src_ref=a_v[1].at[j, rows], dst_ref=a_v[1].at[j, rows],
            send_sem=t_send.at[1, g, k - WHOLE], recv_sem=t_recv.at[1, g, k - WHOLE],
            device_id={'tp': mate}, device_id_type=MESH)

    def pair_sum(ex, ch, k):
        mate_copy(ex, ch, k).wait_recv()
        own = core * HALF_T + k
        a_v[ch][own] = (a_v[ch][own].astype(F32) + p_in[ch][k].astype(F32)).astype(BF16)

    def full_sum(ex, ch, k):
        peer_copy(ex, ch, k).wait()
        own = core * HALF_T + k
        a_v[ch][own] = (a_v[ch][own].astype(F32) + r_v[ex][ch][k].astype(F32)).astype(BF16)
        gather_copy(ex, ch, k, core).start()

    def sends_done(ex, ch):
        def step(k, _):
            gather_copy(ex, ch, k, core).wait_send()
            mate_copy(ex, ch, k).wait_send()
        loop(PIECES, step)

    def gather_done(ex, ch):
        def step(k, _):
            gather_copy(ex, ch, k, 1 - core).wait_recv()
        loop(PIECES, step)
        sends_done(ex, ch)

    def full_sums(ex, ch):
        def step(k, _):
            full_sum(ex, ch, k)
        loop(PIECES, step)

    def norm_add(ch, which, then=None, steps=range(STEPS), squares=None):
        def step(b, _):
            rows = pl.ds(pl.multiple_of(b * NORM_ROWS, NORM_ROWS), NORM_ROWS)
            if squares is None:
                acc = jnp.zeros((NORM_ROWS, PW), F32)
                for j in range(D_TILES):
                    val = a_v[ch][j, rows, :].astype(F32)
                    acc = acc + val * val
            else:
                acc = squares[rows, :]
            fac = lax.rsqrt(jnp.sum(acc, axis=1, keepdims=True) / float(D_MODEL) + NORM_EPS)
            for j in range(D_MODEL // HEAD):
                cols = slice(j * HEAD, (j + 1) * HEAD)
                val = a_v[ch][j * HEAD // PW, rows, j * HEAD % PW:j * HEAD % PW + HEAD].astype(F32)
                base = xh[ch][rows, cols].astype(F32)
                xh[ch][rows, cols] = (base + val * fac * jnp.concatenate([gain_f[which, :, cols]] * (NORM_ROWS // 8))).astype(BF16)
        for t in steps:
            loop((t + 1) * CHUNKS[ch] // NORM_ROWS, step, t * CHUNKS[ch] // NORM_ROWS)
            if then is not None:
                then(t)

    for cp in o_copies + g_copies:
        cp.wait()

    def wo_tile(i, ch):
        rows = pl.ds(pl.multiple_of((i % WO_PER) * Q_W, Q_W), Q_W)
        return jnp.dot(xh[ch][:, pl.ds(0, Q_W)], ring[RING + i // WO_PER, rows, :],
                       preferred_element_type=F32).astype(BF16)

    def wo_sweep(ch):
        def step(k, _):
            if ch == 0:
                wo_copy(2 * k).wait()
                wo_copy(2 * k + 1).wait()

                @pl.when(2 * k + WO_AHEAD < D_TILES)
                def _():
                    wo_copy(2 * k + WO_AHEAD).start()
                    wo_copy(2 * k + WO_AHEAD + 1).start()
            p_out[ch][k] = wo_tile(2 * k, ch)
            mate_copy(0, ch, k).start()
            a_v[ch][core * HALF_T + k] = wo_tile(2 * k + 1, ch)

            pair_sum(0, ch, k)
            if ch == 0:
                peer_copy(0, ch, k).start()
        loop(PIECES, step)

    pl.semaphore_wait(barrier, 2)
    with jax.named_scope('wo'):
        wo_sweep(0)
        for n in range(RING):
            stream(0, n, True)
        for r in range(WO_SLOTS, RESID):
            for cp in res_copies(r):
                cp.start()
        wo_sweep(1)

    for cp in x_copies:
        cp.start()
    for r in range(WO_SLOTS):
        for cp in res_copies(r):
            cp.start()
    with jax.named_scope('sums_a1'):
        def add_squares(val):
            for c in range(0, PW, HEAD):
                part = val[:, c:c + HEAD]
                ssq[...] = ssq[...] + part * part

        def mate_square(k):
            gather_copy(0, 0, k, 1 - core).wait_recv()
            val = a_v[0][(1 - core) * HALF_T + k].astype(F32)
            add_squares(val)

        ssq[...] = jnp.zeros_like(ssq)
        for which, gain_ref in enumerate((ga_ref, gm_ref)):
            for j in range(D_MODEL // HEAD):
                row = gain_ref[j:j + 1, :].astype(F32)
                gain_f[which, :, j * HEAD:(j + 1) * HEAD] = jnp.broadcast_to(row, (8, HEAD))

        def first_sums(k, _):
            full_sum(0, 0, k)
            val = a_v[0][core * HALF_T + k].astype(F32)
            add_squares(val)

            @pl.when(k >= 1)
            def _():
                mate_square(k - 1)

            @pl.when(k >= B_LAG)
            def _():
                peer_copy(0, 1, k - B_LAG).start()
        loop(PIECES, first_sums)
        for k in range(PIECES - B_LAG, PIECES):
            peer_copy(0, 1, k).start()
    with jax.named_scope('gather_a1'):
        mate_square(PIECES - 1)
    for cp in x_copies:
        cp.wait()
    with jax.named_scope('norm_a1'):
        norm_add(0, 0, squares=ssq)
        sends_done(0, 0)

    def gate_up(ph, ch):
        def tile(i, slot):
            acc = jnp.dot(xh[ch][...], ring[slot], preferred_element_type=F32)
            gate = acc[:, :GW]
            act = (gate * jax.nn.sigmoid(gate)) * acc[:, GW:]
            u_v[ch][:, pl.ds(g_col(i), GW)] = act.astype(BF16)

        def single(q, _):
            tile(g_tile(q), stream(ph, q, False))
            refill(ph, q)

        def pair(q, _):
            slot = stream(ph, G_EXTRA + q, False)
            if ph == 0:
                for cp in res_copies(q):
                    cp.wait()
            tile(2 * q, slot)
            tile(2 * q + 1, RING + q)
            refill(ph, G_EXTRA + q)
        loop(G_EXTRA, single)
        loop(RESID, pair)

    def down(ph, ch, also, lag):
        def swap(k):
            pair_sum(1, ch, k)
            peer_copy(1, ch, k).start()

        def d_tile(i):
            slot = stream(ph, i, False)
            res = jnp.dot(u_v[ch][...], ring[slot, pl.ds(0, FF_LOC), :], preferred_element_type=F32).astype(BF16)
            refill(ph, i)
            return res

        def step(k, _):
            also(k)
            p_out[ch][k] = d_tile(2 * k)
            mate_copy(1, ch, k).start()

            if lag:
                @pl.when(k >= 1)
                def _():
                    swap(k - 1)
            a_v[ch][core * HALF_T + k] = d_tile(2 * k + 1)
            if not lag:
                pair_sum(1, ch, k)

                @pl.when(k < WHOLE)
                def _():
                    peer_copy(1, ch, k).start()
        loop(PIECES, step)


    with jax.named_scope('gate_up_a'):
        gate_up(0, 0)
    with jax.named_scope('down_a'):
        down(1, 0, lambda k: full_sum(0, 1, k), True)
    with jax.named_scope('gather_b1'):
        gather_done(0, 1)
    with jax.named_scope('norm_b1'):
        norm_add(1, 0)
        pair_sum(1, 0, PIECES - 1)
        peer_copy(1, 0, PIECES - 1).start()
    with jax.named_scope('gate_up_b'):
        gate_up(2, 1)
    with jax.named_scope('down_b'):
        down(3, 1, lambda k: full_sum(1, 0, k), False)
        for g in PAIR:
            for k in range(WHOLE, PIECES):
                tail_peer(g, k).start()

    def y_copies(ch):
        return [pltpu.make_async_copy(xh[ch].at[pl.ds(t * CHUNKS[ch], CHUNKS[ch]), :],
                                      y_hbm.at[t, pl.ds(firsts[ch], CHUNKS[ch]), :], out_sem.at[ch, t]) for t in range(STEPS)]

    with jax.named_scope('gather_a2'):
        gather_done(1, 0)
    with jax.named_scope('norm_a2'):
        norm_add(0, 1, lambda t: y_copies(0)[t].start())
    with jax.named_scope('sums_b2'):
        def whole_sums(k, _):
            full_sum(1, 1, k)
        loop(WHOLE, whole_sums)
    for g in PAIR:
        rows = pl.ds(*TAIL_ROWS[g])
        with jax.named_scope(f'sums_b2#g={g}'):
            for k in range(WHOLE, PIECES):
                own = core * HALF_T + k
                tail_peer(g, k).wait()
                a_v[1][own, rows, :] = (a_v[1][own, rows, :].astype(F32) + r_v[1][1][k, rows, :].astype(F32)).astype(BF16)
                tail_gather(g, k, core).start()
        with jax.named_scope(f'gather_b2#g={g}'):
            if g == 0:
                def whole_done(k, _):
                    gather_copy(1, 1, k, core).wait_send()
                    gather_copy(1, 1, k, 1 - core).wait_recv()
                loop(WHOLE, whole_done)

                def mates_done(k, _):
                    mate_copy(1, 1, k).wait_send()
                loop(PIECES, mates_done)
            for k in range(WHOLE, PIECES):
                tail_gather(g, k, core).wait_send()
                tail_gather(g, k, 1 - core).wait_recv()
        with jax.named_scope(f'norm_b2#g={g}'):
            norm_add(1, 1, lambda t: y_copies(1)[t].start(), ((0, 1), (2,))[g])
    with jax.named_scope('y_out'):
        for ch in PAIR:
            for cp in y_copies(ch):
                cp.wait()


def run_mlp(o, x_seq, w_o, w_gate, w_up, w_down, g_a, g_m):
    sem = pltpu.SemaphoreType.DMA
    return pl.pallas_call(
        mlp_kernel,
        out_shape=jax.ShapeDtypeStruct((STEPS, BATCH, D_MODEL), BF16),
        in_specs=[HB] * 8,
        out_specs=HB,
        scratch_shapes=[
            *[pltpu.VMEM((n, D_MODEL), BF16) for n in CROWS],
            pltpu.VMEM((max(CROWS), FF_LOC), BF16),
            pltpu.VMEM((CROWS[0], HEAD), F32),
            *[pltpu.VMEM((PIECES, n, PW), BF16) for n in CROWS * 4],
            *[pltpu.VMEM((D_TILES, n, PW), BF16) for n in CROWS],
            pltpu.VMEM((RING + RESID, D_MODEL, PW), BF16),
            *[pltpu.VMEM((D_MODEL // HEAD, HEAD), BF16)] * 2,
            pltpu.VMEM((2, 8, D_MODEL), F32),
            sem((2, 2, STEPS)), sem((2,)), sem((D_TILES,)), sem((RING, 2)), sem((RESID, 2)), sem((2, STEPS)),
            *[sem((2, 2, PIECES))] * 6,
            *[sem((2, 2, PIECES - WHOLE))] * 2,
        ],
        compiler_params=pltpu.CompilerParams(collective_id=1, has_side_effects=True, vmem_limit_bytes=VMEM_ALL),
        name='wo_mlp',
    )(o, x_seq, w_o, w_gate, w_up, w_down, g_a, g_m)


Y_ROWS = 32


def copy_kernel(y_in, y_out, buf, in_sem, out_sem):
    pieces = [(t, pl.ds(r, Y_ROWS)) for t in range(STEPS) for r in range(0, BATCH, Y_ROWS)]
    ins = [pltpu.make_async_copy(y_in.at[p], buf.at[p], in_sem.at[n]) for n, p in enumerate(pieces)]
    outs = [pltpu.make_async_copy(buf.at[p], y_out.at[p], out_sem.at[n]) for n, p in enumerate(pieces)]
    for cp in ins:
        cp.start()
    for came, goes in zip(ins, outs):
        came.wait()
        goes.start()
    for cp in outs:
        cp.wait()


def run_copy(y):
    n = STEPS * BATCH // Y_ROWS
    return pl.pallas_call(
        copy_kernel,
        out_shape=jax.ShapeDtypeStruct(y.shape, BF16),
        in_specs=[HB],
        out_specs=HB,
        scratch_shapes=[pltpu.VMEM(y.shape, BF16), *[pltpu.SemaphoreType.DMA((n,))] * 2],
        compiler_params=pltpu.CompilerParams(vmem_limit_bytes=VMEM_ALL),
        name='place_y',
    )(y)


def solution(mesh):
    def local_run(x_seq, cache_len, k_cache, v_cache, w_q, w_k, w_v, w_o, w_gate, w_up, w_down, g_q, g_k, g_attn, g_mlp):
        inv_freq = ROPE_THETA ** (-(np.arange(HEAD // 2, dtype=np.float32) * np.float32(2.0 / HEAD)))
        freq_row = jnp.asarray(np.concatenate([inv_freq, inv_freq])[None, :], dtype=F32)
        tiled = lambda g: g.reshape(-1, HEAD)
        q_rot, k_new, v_new = run_qkv(x_seq.reshape(ROWS, D_MODEL), w_q, w_k, w_v, tiled(g_q), tiled(g_k), cache_len[None, :], freq_row)
        o, k_out, v_out = run_attn(cache_len, q_rot, k_new, v_new, k_cache, v_cache)
        y = run_mlp(o, x_seq, w_o, w_gate, w_up, w_down, tiled(g_attn), tiled(g_mlp))
        return run_copy(y), k_out, v_out

    data_spec = P(None, 'dp')
    cache_spec = P('dp', 'tp')
    col_spec = P(None, 'tp')
    row_spec = P('tp')
    arg_specs = (data_spec, P('dp'), cache_spec, cache_spec, col_spec, col_spec, col_spec, row_spec, col_spec, col_spec, row_spec, P('tp'), P('tp'), P(), P())
    out_specs = (data_spec, cache_spec, cache_spec)
    return jax.shard_map(local_run, mesh=mesh, in_specs=arg_specs, out_specs=out_specs, check_vma=False)
```
